256 devices in a mesh: row: 4 (over z_hi, core), col: 16 (over z_lo, y), layer: 4 (over x).
Axes of the slice: x: 4, y: 4, z: 8 (z_hi: 2, z_lo: 4; z = z_hi * 4 + z_lo), core: 2. Of those that a mesh axis runs over, the one named last changes fastest.
Arguments:
- amplitudes: float32 [2016, 73536], P('row', ('layer', 'col')), may hold values from -6 to 6
- integrals: float32 [73536, 768], P(('layer', 'col'), 'row'), may hold values from -0.0625 to 0.0625
- occ_energy: float32 [64], replicated, may hold values from -2 to -0.5
- vir_energy: float32 [384], replicated, may hold values from 0.2 to 3
Outputs:
- ladder: float32 [2016, 768], P('col', ('row', 'layer'))
- amplitude_step: float32 [2016, 768], P('col', ('row', 'layer'))
The draws below stay inside these ranges and needn't reach their ends.
All inputs are finite; a program needn't handle non-finite values.
Results may differ from the reference program's by a relative error of at most 0.00007.
Values sent between devices are 32-bit elements; how exact they have to be, the bound alone decides.
A program may use at most 64 MiB of HBM per device.

```python
import jax
import jax.numpy as jnp
import numpy as np
from jax import lax

NO = 64
NV = 384
IJ = 2016
K = 73536
AB = 768


def spiked(values, stream_key, source, target, parts, factor):
    def block_of(dim):
        return (jnp.arange(values.shape[dim]) // (values.shape[dim] // parts)).reshape((-1,) + (1,) * (values.ndim - 1 - dim))

    one_side = jax.random.permutation(stream_key, parts)[block_of(target)]
    far = (block_of(target) + parts // 2) % parts
    return jnp.where((block_of(source) == one_side) | (block_of(source) == far), factor * values, values)


def level_of(stream_key, shape, pieces, low, top_value):
    level, own = 1.0, jax.random.fold_in(stream_key, 6)
    for axis_at, parts in pieces:
        steps = jnp.exp(jax.random.uniform(jax.random.fold_in(own, axis_at), (parts,), jnp.float32, low / len(pieces), top_value / len(pieces)))
        level = level * jnp.repeat(steps, shape[axis_at] // parts).reshape([-1 if axis == axis_at else 1 for axis in range(len(shape))])
    return level


def gaussian(own_key, shape, deviation, limit, shards=(), kind=jnp.bfloat16):
    result = jax.random.normal(own_key, shape, jnp.float32) * deviation
    if len(shards) > 0:
        result = level_of(own_key, shape, shards, -0.22, 0.18) * result
    return jnp.clip(result, min=-limit, max=limit).astype(kind)


def noise_with(key, shape, deviation, reach, split, heavy, kind=jnp.bfloat16):
    values = deviation * jax.random.normal(key, shape, jnp.float32)
    if split:
        values = values * level_of(key, shape, split, -0.22, 0.18)
    return jnp.clip(spiked(values, jax.random.fold_in(key, 3), *heavy), -reach, reach).astype(kind)


def setup_inputs(seed: int = 0) -> dict:
    seeds = jax.random.split(jax.random.key(seed), 5)
    return {
        "amplitudes": gaussian(seeds[0], (IJ, K), 1.0, 6.0, ((0, 4), (1, 64)), jnp.float32),
        "integrals": noise_with(seeds[1], (K, AB), K ** -0.5, 0.0625, ((0, 64), (1, 4)), (0, 1, 64, 4.0), jnp.float32),
        "occ_energy": jnp.clip(jax.random.uniform(seeds[2], (NO,), jnp.float32, -2.0, -0.5), -2.0, -0.5),
        "vir_energy": jnp.clip(jax.random.uniform(seeds[3], (NV,), jnp.float32, 0.2, 3.0), 0.2, 3.0),
    }


def reference(amplitudes, integrals, occ_energy, vir_energy):
    first_np, second_np = np.triu_indices(NO, 1)
    first_index = jnp.asarray(first_np, dtype=jnp.int32)
    second_index = jnp.asarray(second_np, dtype=jnp.int32)
    ladder = jnp.dot(amplitudes, integrals, precision=lax.Precision.HIGHEST, preferred_element_type=jnp.float32)
    pair_sum = occ_energy[first_index] + occ_energy[second_index]
    ab_index = jnp.arange(AB, dtype=jnp.int32)
    vir_sum = vir_energy[ab_index // NV] + vir_energy[ab_index % NV]
    denominator = pair_sum[:, None] - vir_sum[None, :]
    return ladder, ladder / denominator
```

```python
import functools

import jax
import jax.numpy as jnp
from jax import lax
from jax.experimental import pallas as pl
from jax.experimental.pallas import tpu as pltpu
from jax.sharding import PartitionSpec as P

MESH = pl.DeviceIdType.MESH
F32, BF16 = jnp.float32, jnp.bfloat16

OCC, VIR = 64, 384
ROWS = 504
OWN = 126
EF = 1149
KP = 1152
COLS = 192
SLAB = 48
CH = 6
BLK = 128


def split(value):
    high = value.astype(BF16)
    return high, (value - high.astype(F32)).astype(BF16)


def denominators(occ, vir, col, slab_a, slab_b):
    p = lax.broadcasted_iota(jnp.int32, (BLK, OCC), 0) + col * OWN
    i = lax.broadcasted_iota(jnp.int32, (BLK, OCC), 1)
    first = i * (2 * OCC - 1 - i) // 2
    is_i = (p >= first) & (p < first + OCC - 1 - i)
    j = p[:, :1] + jnp.sum(jnp.where(is_i, i + 1 - first, 0), axis=1, keepdims=True)
    row = lambda mask: jnp.sum(jnp.where(mask, occ, 0.0), axis=1, keepdims=True)
    pair_sum = row(is_i) + row(i == j)
    lane = lax.broadcasted_iota(jnp.int32, (1, VIR), 1)
    vir_a = jnp.sum(jnp.where(lane == slab_a, vir, 0.0), axis=1, keepdims=True)
    b = lax.broadcasted_iota(jnp.int32, (SLAB, VIR), 1)
    q = lax.broadcasted_iota(jnp.int32, (SLAB, VIR), 0) + slab_b
    vir_b = jnp.sum(jnp.where(b == q, vir, 0.0), axis=1, keepdims=True)
    vir_sum = jnp.transpose(jnp.broadcast_to(vir_a + vir_b, (SLAB, BLK)))
    return pair_sum - vir_sum


def kernel(
    a_hbm, b_hbm, occ_ref, vir_ref, ladder_ref, step_ref,
    a_own, a_other, b_own, a_high, a_low, chunks, outgoing, incoming, reduced, landed, denom,
    a_sem, b_sem, core_send, core_recv, z_send, z_recv, xy_send, xy_recv, end_send, end_recv,
):
    row, col, x = lax.axis_index("row"), lax.axis_index("col"), lax.axis_index("layer")
    half, core = row // 2, row % 2
    z, y = col // 4, col % 4
    plane = x * 4 + y

    def device(half_to, z_to, y_to, x_to, core_to=core):
        return (half_to * 2 + core_to, z_to * 4 + y_to, x_to)

    load_b = pltpu.make_async_copy(b_hbm, b_own, b_sem)
    load_b.start()
    load_a = pltpu.make_async_copy(a_hbm, a_own, a_sem)
    load_a.start()

    barrier = pltpu.get_barrier_semaphore()

    def greet(to):
        pl.semaphore_signal(barrier, inc=1, device_id=to, device_id_type=MESH)

    greet(device(half, z, y, x, 1 - core))
    for step in range(1, 8):
        to = lax.rem(half * 4 + z + step, 8)
        greet(device(to // 4, to % 4, y, x))
    for step in range(1, 16):
        to = lax.rem(plane + step, 16)
        greet(device(half, z, to % 4, to // 4))

    load_b.wait()
    for block in range(KP // BLK):
        lanes = pl.ds(block * BLK, BLK)
        if block < KP // BLK - 1:
            part = b_own[lanes, :]
        else:
            part = pltpu.roll(b_own[pl.ds(EF - BLK, BLK), :], BLK - (KP - EF), 0)
            k = lax.broadcasted_iota(jnp.int32, part.shape, 0) + block * BLK
            part = jnp.where(k < EF, part, 0.0)
        part = jnp.transpose(part)
        for owner in range(4):
            for c in range(CH):
                at = owner * SLAB + c * 8
                chunks[c, owner, :, lanes] = part[at : at + 8, :]

    pl.semaphore_wait(barrier, 23)

    def z_copy(c):
        return pltpu.make_async_remote_copy(
            chunks.at[c], chunks.at[CH + c], z_send.at[c], z_recv.at[c],
            device_id=device(1 - half, z, y, x), device_id_type=MESH,
        )

    for c in range(CH):
        z_copy(c).start()

    load_a.wait()
    a_copy = pltpu.make_async_remote_copy(
        a_own, a_other, core_send, core_recv,
        device_id=device(half, z, y, x, 1 - core), device_id_type=MESH,
    )
    a_copy.start()

    def prepare(source, which):
        def block_of(block, masked):
            at = block * BLK if masked else pl.multiple_of(block * BLK, BLK)
            for owner in range(4):
                lanes = pl.ds(at, EF - at if masked else BLK)
                if owner < 3:
                    part = source[pl.ds(owner * OWN, BLK), lanes]
                else:
                    part = pltpu.roll(source[pl.ds(ROWS - BLK, BLK), lanes], OWN, 0)
                if masked:
                    part = jnp.pad(part, ((0, 0), (0, KP - EF)))
                high, low = split(jnp.transpose(part))
                lanes = pl.ds(owner * 256 + which * BLK, BLK)
                a_high[pl.ds(at, BLK), lanes] = high
                a_low[pl.ds(at, BLK), lanes] = low

        @pl.loop(0, KP // BLK - 1)
        def _(block):
            block_of(block, False)

        block_of(KP // BLK - 1, True)

    prepare(a_own, 0)
    denom[...] = denominators(occ_ref[...], vir_ref[...], col, half, core * COLS + x * SLAB)
    a_copy.wait_recv()
    prepare(a_other, 1)

    def xy_copy(c, to):
        return pltpu.make_async_remote_copy(
            outgoing.at[c, to], incoming.at[c, plane], xy_send.at[c], xy_recv.at[c],
            device_id=device(half, z, to % 4, to // 4), device_id_type=MESH,
        )

    def end_copy(c, which, half_to):
        z_to = 2 * half + lax.rem(core + which, 2)
        return z_to, pltpu.make_async_remote_copy(
            reduced.at[c, which], landed.at[lax.rem(c, CH), z], end_send, end_recv,
            device_id=device(half_to, z_to, y, x), device_id_type=MESH,
        )

    def multiply(c):
        b_high, b_low = split(chunks[c].reshape(32, KP))
        both = jnp.concatenate([b_high, b_low], axis=0)
        upper = jnp.dot(both, a_high[...], preferred_element_type=F32)
        lower = jnp.dot(b_high, a_low[...], preferred_element_type=F32)
        value = upper[:32] + (upper[32:] + lower)
        for x_to in range(4):
            for y_to in range(4):
                outgoing[c, x_to * 4 + y_to] = value[8 * x_to : 8 * x_to + 8, 256 * y_to : 256 * y_to + 256]
        incoming[c, plane] = outgoing[c, plane]

        @pl.loop(1, 16)
        def _(step):
            xy_copy(c, lax.rem(plane + step, 16)).start()

    def reduce(c, cross):
        xy_all = pltpu.make_async_remote_copy(
            outgoing.at[c, pl.ds(0, 15)], incoming.at[c, pl.ds(0, 15)], xy_send.at[c], xy_recv.at[c],
            device_id=device(1 - half, z, y, x), device_id_type=MESH,
        )
        xy_all.wait_recv()
        total = jnp.sum(incoming[c], axis=0)
        for which in range(2):
            reduced[c, which] = total[:, which * BLK : which * BLK + BLK]
        for which in range(2):
            z_to, copy = end_copy(c, which, 1 - half if cross else half)
            if cross:
                copy.start()
            else:

                @pl.when(z_to == z)
                def _():
                    landed[lax.rem(c, CH), z] = reduced[c, which]

                @pl.when(z_to != z)
                def _():
                    copy.start()

    @pl.loop(0, 2 * CH)
    def _(c):
        @pl.when(c >= CH)
        def _():
            z_copy(c - CH).wait_recv()

        multiply(c)

        @pl.when(c >= CH)
        def _():
            reduce(c - CH, False)

        @pl.when(c > CH)
        def _():
            reduce(c - 1, True)

    reduce(2 * CH - 1, True)

    def end_all(count):
        return pltpu.make_async_remote_copy(
            landed.at[:, pl.ds(0, count)], landed.at[:, pl.ds(0, count)], end_send, end_recv,
            device_id=device(1 - half, z, y, x), device_id_type=MESH,
        )

    home = z // 2 == half

    @pl.when(home)
    def _():
        end_all(3).wait_recv()

    @pl.when(jnp.logical_not(home))
    def _():
        end_all(4).wait_recv()

    total = jnp.sum(landed[...], axis=1).reshape(SLAB, BLK)
    ladder = jnp.transpose(total)[:OWN, :]
    ladder_ref[...] = ladder
    step_ref[...] = ladder / denom[:OWN, :]

    a_copy.wait_send()
    for c in range(CH):
        z_copy(c).wait_send()

    @pl.loop(0, 2 * CH)
    def _(c):
        pltpu.make_async_remote_copy(
            outgoing.at[c, pl.ds(0, 15)], incoming.at[c, pl.ds(0, 15)], xy_send.at[c], xy_recv.at[c],
            device_id=device(1 - half, z, y, x), device_id_type=MESH,
        ).wait_send()

    end_all(3).wait_send()

    @pl.when(jnp.logical_not(home))
    def _():
        landed_one = landed.at[:, pl.ds(0, 1)]
        pltpu.make_async_remote_copy(
            landed_one, landed_one, end_send, end_recv,
            device_id=device(1 - half, z, y, x), device_id_type=MESH,
        ).wait_send()


def shards(amplitudes, integrals, occ_energy, vir_energy):
    block = jax.ShapeDtypeStruct((OWN, SLAB), F32)
    dma = pltpu.SemaphoreType.DMA
    vmem = pl.BlockSpec(memory_space=pltpu.VMEM)
    hbm = pl.BlockSpec(memory_space=pl.ANY)
    return pl.pallas_call(
        kernel,
        out_shape=(block, block),
        in_specs=[hbm, hbm, vmem, vmem],
        out_specs=(vmem, vmem),
        scratch_shapes=[
            pltpu.VMEM((ROWS, EF), F32),
            pltpu.VMEM((ROWS, EF), F32),
            pltpu.VMEM((EF, COLS), F32),
            pltpu.VMEM((KP, 1024), BF16),
            pltpu.VMEM((KP, 1024), BF16),
            pltpu.VMEM((2 * CH, 4, 8, KP), F32),
            pltpu.VMEM((2 * CH, 16, 8, 256), F32),
            pltpu.VMEM((2 * CH, 16, 8, 256), F32),
            pltpu.VMEM((2 * CH, 2, 8, BLK), F32),
            pltpu.VMEM((CH, 4, 8, BLK), F32),
            pltpu.VMEM((BLK, SLAB), F32),
            dma, dma, dma, dma,
            dma((CH,)), dma((CH,)),
            dma((2 * CH,)), dma((2 * CH,)),
            dma, dma,
        ],
        compiler_params=pltpu.CompilerParams(collective_id=0, has_side_effects=True, vmem_limit_bytes=56 * 2**20),
    )(amplitudes, integrals, occ_energy.reshape(1, OCC), vir_energy.reshape(1, VIR))


def solution(mesh):
    in_specs = (P("row", ("layer", "col")), P(("layer", "col"), "row"), P(), P())
    out_specs = (P("col", ("row", "layer")), P("col", ("row", "layer")))
    return jax.shard_map(shards, mesh=mesh, in_specs=in_specs, out_specs=out_specs, check_vma=False)
```

```python
import functools

import jax
import jax.numpy as jnp
from jax import lax
from jax.experimental import pallas as pl
from jax.experimental.pallas import tpu as pltpu
from jax.sharding import PartitionSpec as P

MESH = pl.DeviceIdType.MESH
F32, BF16 = jnp.float32, jnp.bfloat16

OCC, VIR = 64, 384
ROWS = 504
OWN = 126
EF = 1149
KP = 1152
COLS = 192
SLAB = 48
CH = 6
BLK = 128


def split(value):
    high = value.astype(BF16)
    return high, (value - high.astype(F32)).astype(BF16)


def denominators(occ, vir, col, slab_a, slab_b):
    p = lax.broadcasted_iota(jnp.int32, (BLK, OCC), 0) + col * OWN
    i = lax.broadcasted_iota(jnp.int32, (BLK, OCC), 1)
    first = i * (2 * OCC - 1 - i) // 2
    is_i = (p >= first) & (p < first + OCC - 1 - i)
    j = p[:, :1] + jnp.sum(jnp.where(is_i, i + 1 - first, 0), axis=1, keepdims=True)
    row = lambda mask: jnp.sum(jnp.where(mask, occ, 0.0), axis=1, keepdims=True)
    pair_sum = row(is_i) + row(i == j)
    lane = lax.broadcasted_iota(jnp.int32, (1, VIR), 1)
    vir_a = jnp.sum(jnp.where(lane == slab_a, vir, 0.0), axis=1, keepdims=True)
    b = lax.broadcasted_iota(jnp.int32, (SLAB, VIR), 1)
    q = lax.broadcasted_iota(jnp.int32, (SLAB, VIR), 0) + slab_b
    vir_b = jnp.sum(jnp.where(b == q, vir, 0.0), axis=1, keepdims=True)
    return jnp.transpose(jnp.broadcast_to(pair_sum, (BLK, BLK)))[:SLAB] - (vir_a + vir_b)


def kernel(
    a_hbm, b_hbm, occ_ref, vir_ref, ladder_ref, denom_ref,
    a_own, a_other, a_high, a_low, chunks, outgoing, incoming, reduced, landed,
    a_sem, b_sem, core_send, core_recv, z_send, z_recv, xy_send, xy_recv, end_send, end_recv,
):
    row, col, x = lax.axis_index("row"), lax.axis_index("col"), lax.axis_index("layer")
    half, core = row // 2, row % 2
    z, y = col // 4, col % 4
    plane = x * 4 + y

    def device(half_to, z_to, y_to, x_to, core_to=core):
        return (half_to * 2 + core_to, z_to * 4 + y_to, x_to)

    loads = [
        pltpu.make_async_copy(b_hbm.at[:, pl.ds(8 * c, 8), :], chunks.at[c], b_sem.at[c]) for c in range(CH)
    ]
    for load in loads:
        load.start()
    load_a = pltpu.make_async_copy(a_hbm, a_own, a_sem)
    load_a.start()

    barrier = pltpu.get_barrier_semaphore()

    def greet(to):
        pl.semaphore_signal(barrier, inc=1, device_id=to, device_id_type=MESH)

    greet(device(half, z, y, x, 1 - core))
    for step in range(1, 8):
        to = lax.rem(half * 4 + z + step, 8)
        greet(device(to // 4, to % 4, y, x))
    for step in range(1, 16):
        to = lax.rem(plane + step, 16)
        greet(device(half, z, to % 4, to // 4))

    pl.semaphore_wait(barrier, 23)

    def z_copy(c):
        return pltpu.make_async_remote_copy(
            chunks.at[c], chunks.at[CH + c], z_send.at[c], z_recv.at[c],
            device_id=device(1 - half, z, y, x), device_id_type=MESH,
        )

    for c in range(CH):
        loads[c].wait()
        z_copy(c).start()

    load_a.wait()
    a_copy = pltpu.make_async_remote_copy(
        a_own, a_other, core_send, core_recv,
        device_id=device(half, z, y, x, 1 - core), device_id_type=MESH,
    )
    a_copy.start()

    def prepare(source, which):
        def block_of(block, masked):
            at = block * BLK if masked else pl.multiple_of(block * BLK, BLK)
            for owner in range(4):
                lanes = pl.ds(at, EF - at if masked else BLK)
                if owner < 3:
                    part = source[pl.ds(owner * OWN, BLK), lanes]
                else:
                    part = pltpu.roll(source[pl.ds(ROWS - BLK, BLK), lanes], OWN, 0)
                if masked:
                    part = jnp.pad(part, ((0, 0), (0, KP - EF)))
                high, low = split(jnp.transpose(part))
                lanes = pl.ds(owner * 256 + which * BLK, BLK)
                a_high[pl.ds(at, BLK), lanes] = high
                a_low[pl.ds(at, BLK), lanes] = low

        @pl.loop(0, KP // BLK - 1)
        def _(block):
            block_of(block, False)

        block_of(KP // BLK - 1, True)

    prepare(a_own, 0)
    denom_ref[...] = denominators(occ_ref[...].reshape(1, OCC), vir_ref[...].reshape(1, VIR), col, half, core * COLS + x * SLAB)
    a_copy.wait_recv()
    prepare(a_other, 1)

    def xy_copy(c, to):
        return pltpu.make_async_remote_copy(
            outgoing.at[c, to], incoming.at[c, plane], xy_send.at[c], xy_recv.at[c],
            device_id=device(half, z, to % 4, to // 4), device_id_type=MESH,
        )

    def end_copy(c, which, half_to):
        z_to = 2 * half + lax.rem(core + which, 2)
        return z_to, pltpu.make_async_remote_copy(
            reduced.at[c, which], landed.at[lax.rem(c, CH), z], end_send, end_recv,
            device_id=device(half_to, z_to, y, x), device_id_type=MESH,
        )

    def multiply(c):
        b_high, b_low = split(jnp.pad(chunks[c].reshape(32, EF), ((0, 0), (0, KP - EF))))
        both = jnp.concatenate([b_high, b_low], axis=0)
        upper = jnp.dot(both, a_high[...], preferred_element_type=F32)
        lower = jnp.dot(b_high, a_low[...], preferred_element_type=F32)
        value = upper[:32] + (upper[32:] + lower)
        for x_to in range(4):
            for y_to in range(4):
                outgoing[c, x_to * 4 + y_to] = value[8 * x_to : 8 * x_to + 8, 256 * y_to : 256 * y_to + 256]
        incoming[c, plane] = outgoing[c, plane]

        @pl.loop(1, 16)
        def _(step):
            xy_copy(c, lax.rem(plane + step, 16)).start()

    def reduce(c, cross):
        xy_all = pltpu.make_async_remote_copy(
            outgoing.at[c, pl.ds(0, 15)], incoming.at[c, pl.ds(0, 15)], xy_send.at[c], xy_recv.at[c],
            device_id=device(1 - half, z, y, x), device_id_type=MESH,
        )
        xy_all.wait_recv()
        total = jnp.sum(incoming[c], axis=0)
        for which in range(2):
            reduced[c, which] = total[:, which * BLK : which * BLK + BLK]
        for which in range(2):
            z_to, copy = end_copy(c, which, 1 - half if cross else half)
            if cross:
                copy.start()
            else:

                @pl.when(z_to == z)
                def _():
                    landed[lax.rem(c, CH), z] = reduced[c, which]

                @pl.when(z_to != z)
                def _():
                    copy.start()

    @pl.loop(0, 2 * CH)
    def _(c):
        @pl.when(c >= CH)
        def _():
            z_copy(c - CH).wait_recv()

        multiply(c)

        @pl.when(c >= CH)
        def _():
            reduce(c - CH, False)

        @pl.when(c > CH)
        def _():
            reduce(c - 1, True)

    reduce(2 * CH - 1, True)

    def end_all(count):
        return pltpu.make_async_remote_copy(
            landed.at[:, pl.ds(0, count)], landed.at[:, pl.ds(0, count)], end_send, end_recv,
            device_id=device(1 - half, z, y, x), device_id_type=MESH,
        )

    home = z // 2 == half

    @pl.when(home)
    def _():
        end_all(3).wait_recv()

    @pl.when(jnp.logical_not(home))
    def _():
        end_all(4).wait_recv()

    ladder_ref[...] = jnp.sum(landed[...], axis=1).reshape(SLAB, BLK)

    a_copy.wait_send()
    for c in range(CH):
        z_copy(c).wait_send()

    @pl.loop(0, 2 * CH)
    def _(c):
        pltpu.make_async_remote_copy(
            outgoing.at[c, pl.ds(0, 15)], incoming.at[c, pl.ds(0, 15)], xy_send.at[c], xy_recv.at[c],
            device_id=device(1 - half, z, y, x), device_id_type=MESH,
        ).wait_send()

    end_all(3).wait_send()

    @pl.when(jnp.logical_not(home))
    def _():
        landed_one = landed.at[:, pl.ds(0, 1)]
        pltpu.make_async_remote_copy(
            landed_one, landed_one, end_send, end_recv,
            device_id=device(1 - half, z, y, x), device_id_type=MESH,
        ).wait_send()


def shards(amplitudes, integrals, occ_energy, vir_energy):
    block = jax.ShapeDtypeStruct((SLAB, BLK), F32)
    dma = pltpu.SemaphoreType.DMA
    vmem = pl.BlockSpec(memory_space=pltpu.VMEM)
    hbm = pl.BlockSpec(memory_space=pl.ANY)
    ladder, denominator = pl.pallas_call(
        kernel,
        out_shape=(block, block),
        in_specs=[hbm, hbm, vmem, vmem],
        out_specs=(vmem, vmem),
        scratch_shapes=[
            pltpu.VMEM((ROWS, EF), F32),
            pltpu.VMEM((ROWS, EF), F32),
            pltpu.VMEM((KP, 1024), BF16),
            pltpu.VMEM((KP, 1024), BF16),
            pltpu.VMEM((2 * CH, 4, 8, EF), F32),
            pltpu.VMEM((2 * CH, 16, 8, 256), F32),
            pltpu.VMEM((2 * CH, 16, 8, 256), F32),
            pltpu.VMEM((2 * CH, 2, 8, BLK), F32),
            pltpu.VMEM((CH, 4, 8, BLK), F32),
                        dma, dma((CH,)), dma, dma,
            dma((CH,)), dma((CH,)),
            dma((2 * CH,)), dma((2 * CH,)),
            dma, dma,
        ],
        compiler_params=pltpu.CompilerParams(collective_id=0, has_side_effects=True, vmem_limit_bytes=56 * 2**20),
    )(amplitudes, integrals.T.reshape(4, SLAB, EF), occ_energy, vir_energy)
    ladder = ladder[:, :OWN].T
    return ladder, ladder / denominator[:, :OWN].T


def solution(mesh):
    in_specs = (P("row", ("layer", "col")), P(("layer", "col"), "row"), P(), P())
    out_specs = (P("col", ("row", "layer")), P("col", ("row", "layer")))
    return jax.shard_map(shards, mesh=mesh, in_specs=in_specs, out_specs=out_specs, check_vma=False)
```

```python
import jax
import jax.numpy as jnp
from jax import lax
from jax.experimental import pallas as pl
from jax.experimental.pallas import tpu as pltpu
from jax.sharding import PartitionSpec as P

MESH = pl.DeviceIdType.MESH
F32, BF16 = jnp.float32, jnp.bfloat16

OCC, VIR = 64, 384
ROWS = 504
OWN = 126
EF = 1149
KP = 1152
COLS = 192
SLAB = 48
BLK = 128
TILE = 8
WIDE = 2 * BLK
HALVES = ((0, 3), (3, 3))
LAST = ((0, 3), (3, 2), (5, 1))
PIECES = 9
HELD = 6
LOCAL = PIECES


def far_first(i):
    return jnp.where(i == 0, 2, jnp.where(i == 1, 1, jnp.where(i == 2, 3, 0)))


def split(value):
    high = value.astype(BF16)
    return high, (value - high.astype(F32)).astype(BF16)


def denominators(occ, vir, col, slab_a, slab_b):
    p = lax.broadcasted_iota(jnp.int32, (BLK, OCC), 0) + col * OWN
    i = lax.broadcasted_iota(jnp.int32, (BLK, OCC), 1)
    first = i * (2 * OCC - 1 - i) // 2
    is_i = (p >= first) & (p < first + OCC - 1 - i)
    j = p[:, :1] + jnp.sum(jnp.where(is_i, i + 1 - first, 0), axis=1, keepdims=True)
    row = lambda mask: jnp.sum(jnp.where(mask, occ, 0.0), axis=1, keepdims=True)
    pair_sum = row(is_i) + row(i == j)
    lane = lax.broadcasted_iota(jnp.int32, (1, VIR), 1)
    vir_a = jnp.sum(jnp.where(lane == slab_a, vir, 0.0), axis=1, keepdims=True)
    b = lax.broadcasted_iota(jnp.int32, (SLAB, VIR), 1)
    q = lax.broadcasted_iota(jnp.int32, (SLAB, VIR), 0) + slab_b
    vir_b = jnp.sum(jnp.where(b == q, vir, 0.0), axis=1, keepdims=True)
    return jnp.transpose(jnp.broadcast_to(pair_sum, (BLK, BLK)))[:SLAB] - (vir_a + vir_b)


def kernel(
    a_hbm, b_hbm, occ_ref, vir_ref, ladder_ref, denom_ref,
    a_own, a_other, a_high, a_low, b_own, b_far, outgoing, incoming, partial, reduced, landed,
    a_sem, b_sem, core_send, core_recv, z_send, z_recv, xy_send, xy_recv, end_send, end_recv,
):
    row, col, x = lax.axis_index("row"), lax.axis_index("col"), lax.axis_index("layer")
    half, core = row // 2, row % 2
    z, y = col // 4, col % 4
    plane = x * 4 + y
    far = 1 - half

    def device(half_to, z_to, y_to, x_to, core_to=core):
        return (half_to * 2 + core_to, z_to * 4 + y_to, x_to)

    def remote(src, dst, send, recv, to):
        return pltpu.make_async_remote_copy(src, dst, send, recv, device_id=to, device_id_type=MESH)

    load_b = pltpu.make_async_copy(b_hbm, b_own, b_sem)
    load_b.start()
    load_a = pltpu.make_async_copy(a_hbm, a_own, a_sem)
    load_a.start()

    barrier = pltpu.get_barrier_semaphore()

    def greet(to):
        pl.semaphore_signal(barrier, inc=1, device_id=to, device_id_type=MESH)

    greet(device(half, z, y, x, 1 - core))
    for step in range(1, 8):
        to = lax.rem(half * 4 + z + step, 8)
        greet(device(to // 4, to % 4, y, x))
    for step in range(1, 16):
        to = lax.rem(plane + step, 16)
        greet(device(half, z, to % 4, to // 4))

    load_b.wait()
    pl.semaphore_wait(barrier, 23)

    def z_copy(m, distance, first, tiles):
        at = (lax.rem(x + distance, 4), pl.ds(first * TILE, tiles * TILE))
        return remote(b_own.at[at], b_far.at[at], z_send.at[m], z_recv.at[m], device(far, z, y, x))

    z_copies = [
        z_copy(2 * i + j, (2, 1, 3, 0)[i], *piece)
        for i in range(4)
        for j, piece in enumerate(HALVES if i < 3 else LAST)
    ]
    for copy in z_copies[:HELD]:
        copy.start()

    @pl.when(core == 0)
    def _():
        for copy in z_copies[HELD:]:
            copy.start()

    load_a.wait()
    a_copy = remote(a_own, a_other, core_send, core_recv, device(half, z, y, x, 1 - core))
    a_copy.start()

    def prepare(source, which):
        def block_of(block, masked):
            at = block * BLK if masked else pl.multiple_of(block * BLK, BLK)
            for owner in range(4):
                lanes = pl.ds(at, EF - at if masked else BLK)
                if owner < 3:
                    part = source[pl.ds(owner * OWN, BLK), lanes]
                else:
                    part = pltpu.roll(source[pl.ds(ROWS - BLK, BLK), lanes], OWN, 0)
                if masked:
                    part = jnp.pad(part, ((0, 0), (0, KP - EF)))
                high, low = split(jnp.transpose(part))
                lanes = pl.ds(owner * WIDE + which * BLK, BLK)
                a_high[pl.ds(at, BLK), lanes] = high
                a_low[pl.ds(at, BLK), lanes] = low

        @pl.loop(0, KP // BLK - 1)
        def _(block):
            block_of(block, False)

        block_of(KP // BLK - 1, True)

    prepare(a_own, 0)
    denom_ref[...] = denominators(occ_ref[...].reshape(1, OCC), vir_ref[...].reshape(1, VIR), col, half, core * COLS + x * SLAB)
    a_copy.wait_recv()
    prepare(a_other, 1)

    def multiply(source, kind, m, distance, first, tiles):
        x_to = lax.rem(x + distance, 4)
        at = first * TILE
        if not isinstance(at, int):
            at = pl.multiple_of(at, TILE)
        cols = pl.ds(at, tiles * TILE)
        b = jnp.pad(source[x_to, cols, :], ((0, 0), (0, KP - EF)))
        b_high = b.astype(BF16).astype(F32)
        both = jnp.concatenate([b_high, b - b_high], axis=0).astype(BF16)
        for step in (2, 1, 3, 0):
            y_to = lax.rem(y + step, 4)
            lanes = pl.ds(pl.multiple_of(y_to * WIDE, WIDE), WIDE)
            upper = jnp.dot(both, a_high[:, lanes], preferred_element_type=F32)
            lower = jnp.dot(both, a_low[:, lanes], preferred_element_type=F32)
            n = tiles * TILE
            outgoing[kind, x_to, y_to, cols, :] = upper[:n] + (upper[n:] + (lower[:n] + lower[n:]))

            def send():
                remote(
                    outgoing.at[kind, x_to, y_to, cols], incoming.at[kind, plane, cols],
                    xy_send.at[m], xy_recv.at[m], device(half, z, y_to, x_to),
                ).start()

            if step:
                send()
            elif isinstance(distance, int):
                incoming[kind, plane, cols, :] = outgoing[kind, x_to, y_to, cols, :]
            else:

                @pl.when(distance == 0)
                def _():
                    incoming[kind, plane, cols, :] = outgoing[kind, x_to, y_to, cols, :]

                @pl.when(distance != 0)
                def _():
                    send()

    def xy_all(kind, m, tiles, count):
        blocks = (kind, pl.ds(0, count), pl.ds(0, tiles * TILE))
        return remote(incoming.at[blocks], incoming.at[blocks], xy_send.at[m], xy_recv.at[m], device(far, z, y, x))

    def end_copy(kind, which, cols):
        z_to = 2 * half + lax.rem(core + which, 2)
        half_to = far if kind else half
        return z_to, lambda: remote(
            reduced.at[kind, which, cols], landed.at[z, cols], end_send, end_recv, device(half_to, z_to, y, x)
        ).start()

    @pl.loop(0, 4)
    def _(i):
        multiply(b_own, 0, LOCAL + i, far_first(i), 0, 6)

    def finish_local():
        for i in range(4):
            xy_all(0, LOCAL + i, 6, 4 if i < 3 else 3).wait_recv()
        total = jnp.sum(incoming[0], axis=0)
        for which in range(2):
            reduced[0, which] = total[:, which * BLK : which * BLK + BLK]
        for which in range(2):
            z_to, send = end_copy(0, which, pl.ds(0, SLAB))

            @pl.when(z_to == z)
            def _():
                landed[z] = reduced[0, which]

            @pl.when(z_to != z)
            def _():
                send()

    @pl.loop(0, 7)
    def _(m):
        i = m // 2
        z_copy(m, far_first(i), 0, 3).wait_recv()
        @pl.when((core == 1) & (m == HELD - 1))
        def _():
            for copy in z_copies[HELD:]:
                copy.start()

        multiply(b_far, 1, m, far_first(i), 3 * lax.rem(m, 2), 3)

        @pl.when(m == 2)
        def _():
            finish_local()

    def slot(step):
        return lax.rem(x + step, 4) * 4

    for m in range(6):
        xy_all(1, m, 3, 4).wait_recv()
    total = jnp.sum(incoming[1, pl.ds(slot(1), 4)], axis=0)
    for step in (2, 3):
        total += jnp.sum(incoming[1, pl.ds(slot(step), 4)], axis=0)
    partial[...] = total

    def finish(j):
        first, tiles = LAST[j]
        cols = pl.ds(first * TILE, tiles * TILE)
        xy_all(1, 6 + j, tiles, 3).wait_recv()
        total = partial[cols, :] + jnp.sum(incoming[1, pl.ds(slot(0), 4), cols], axis=0)
        for which in range(2):
            reduced[1, which, cols, :] = total[:, which * BLK : which * BLK + BLK]
            end_copy(1, which, cols)[1]()

    for j in (1, 2):
        z_copies[6 + j].wait_recv()
        multiply(b_far, 1, 6 + j, 0, *LAST[j])
        if j == 1:
            finish(0)
    finish(1)
    finish(2)

    def end_all(count):
        blocks = landed.at[pl.ds(0, count)]
        return remote(blocks, blocks, end_send, end_recv, device(far, z, y, x))

    home = z // 2 == half

    @pl.when(home)
    def _():
        end_all(3).wait_recv()

    @pl.when(jnp.logical_not(home))
    def _():
        end_all(4).wait_recv()

    ladder_ref[...] = jnp.sum(landed[...], axis=0)

    a_copy.wait_send()
    for copy in z_copies:
        copy.wait_send()
    for m in range(PIECES):
        xy_all(1, m, 3 if m < 6 else LAST[m - 6][1], 4 if m < 6 else 3).wait_send()
    for i in range(4):
        xy_all(0, LOCAL + i, 6, 4 if i < 3 else 3).wait_send()
    end_all(3).wait_send()

    @pl.when(jnp.logical_not(home))
    def _():
        end_all(1).wait_send()


def shards(amplitudes, integrals, occ_energy, vir_energy):
    block = jax.ShapeDtypeStruct((SLAB, BLK), F32)
    dma = pltpu.SemaphoreType.DMA
    vmem = pl.BlockSpec(memory_space=pltpu.VMEM)
    hbm = pl.BlockSpec(memory_space=pl.ANY)
    ladder, denominator = pl.pallas_call(
        kernel,
        out_shape=(block, block),
        in_specs=[hbm, hbm, vmem, vmem],
        out_specs=(vmem, vmem),
        scratch_shapes=[
            pltpu.VMEM((ROWS, EF), F32),
            pltpu.VMEM((ROWS, EF), F32),
            pltpu.VMEM((KP, 4 * WIDE), BF16),
            pltpu.VMEM((KP, 4 * WIDE), BF16),
            pltpu.VMEM((4, SLAB, EF), F32),
            pltpu.VMEM((4, SLAB, EF), F32),
            pltpu.VMEM((2, 4, 4, SLAB, WIDE), F32),
            pltpu.VMEM((2, 16, SLAB, WIDE), F32),
            pltpu.VMEM((SLAB, WIDE), F32),
            pltpu.VMEM((2, 2, SLAB, BLK), F32),
            pltpu.VMEM((4, SLAB, BLK), F32),
            dma, dma, dma, dma,
            dma((PIECES,)), dma((PIECES,)),
            dma((PIECES + 4,)), dma((PIECES + 4,)),
            dma, dma,
        ],
        compiler_params=pltpu.CompilerParams(collective_id=0, has_side_effects=True, vmem_limit_bytes=56 * 2**20),
    )(amplitudes, integrals.T.reshape(4, SLAB, EF), occ_energy, vir_energy)
    ladder = ladder[:, :OWN].T
    return ladder, ladder / denominator[:, :OWN].T


def solution(mesh):
    in_specs = (P("row", ("layer", "col")), P(("layer", "col"), "row"), P(), P())
    out_specs = (P("col", ("row", "layer")), P("col", ("row", "layer")))
    return jax.shard_map(shards, mesh=mesh, in_specs=in_specs, out_specs=out_specs, check_vma=False)
```

```python
import jax
import jax.numpy as jnp
from jax import lax
from jax.experimental import pallas as pl
from jax.experimental.pallas import tpu as pltpu
from jax.sharding import PartitionSpec as P

MESH = pl.DeviceIdType.MESH
F32, BF16 = jnp.float32, jnp.bfloat16

OCC, VIR = 64, 384
ROWS = 504
OWN = 126
EF = 1149
KP = 1152
COLS = 192
SLAB = 48
BLK = 128
TILE = 8
WIDE = 2 * BLK
HALVES = ((0, 3), (3, 3))
LAST = ((0, 3), (3, 2), (5, 1))
PIECES = 9
HELD = 6
LOCAL = PIECES


def far_first(i):
    return jnp.where(i == 0, 2, jnp.where(i == 1, 1, jnp.where(i == 2, 3, 0)))


def split(value):
    high = value.astype(BF16)
    return high, (value - high.astype(F32)).astype(BF16)


def denominators(occ, vir, col, slab_a, slab_b):
    p = lax.broadcasted_iota(jnp.int32, (BLK, OCC), 0) + col * OWN
    i = lax.broadcasted_iota(jnp.int32, (BLK, OCC), 1)
    first = i * (2 * OCC - 1 - i) // 2
    is_i = (p >= first) & (p < first + OCC - 1 - i)
    j = p[:, :1] + jnp.sum(jnp.where(is_i, i + 1 - first, 0), axis=1, keepdims=True)
    row = lambda mask: jnp.sum(jnp.where(mask, occ, 0.0), axis=1, keepdims=True)
    pair_sum = row(is_i) + row(i == j)
    lane = lax.broadcasted_iota(jnp.int32, (1, VIR), 1)
    vir_a = jnp.sum(jnp.where(lane == slab_a, vir, 0.0), axis=1, keepdims=True)
    b = lax.broadcasted_iota(jnp.int32, (SLAB, VIR), 1)
    q = lax.broadcasted_iota(jnp.int32, (SLAB, VIR), 0) + slab_b
    vir_b = jnp.sum(jnp.where(b == q, vir, 0.0), axis=1, keepdims=True)
    return jnp.transpose(jnp.broadcast_to(pair_sum, (BLK, BLK)))[:SLAB] - (vir_a + vir_b)


def kernel(
    a_hbm, b_hbm, occ_hbm, vir_hbm, ladder_ref, denom_ref,
    a_own, a_other, a_high, a_low, b_own, b_far, outgoing, incoming, partial, reduced, landed, occ_ref, vir_ref,
    a_sem, b_sem, e_sem, core_send, core_recv, z_send, z_recv, xy_send, xy_recv, end_send, end_recv,
):
    row, col, x = lax.axis_index("row"), lax.axis_index("col"), lax.axis_index("layer")
    half, core = row // 2, row % 2
    z, y = col // 4, col % 4
    plane = x * 4 + y
    far = 1 - half

    def device(half_to, z_to, y_to, x_to, core_to=core):
        return (half_to * 2 + core_to, z_to * 4 + y_to, x_to)

    def remote(src, dst, send, recv, to):
        return pltpu.make_async_remote_copy(src, dst, send, recv, device_id=to, device_id_type=MESH)

    loads = []
    for i, distance in enumerate((2, 1, 3, 0)):
        owner = lax.rem(x + distance, 4)
        loads.append(pltpu.make_async_copy(b_hbm.at[owner], b_own.at[owner], b_sem.at[i]))
        loads[i].start()
    load_a = pltpu.make_async_copy(a_hbm, a_own, a_sem)
    load_a.start()
    load_e = [
        pltpu.make_async_copy(occ_hbm, occ_ref, e_sem.at[0]), pltpu.make_async_copy(vir_hbm, vir_ref, e_sem.at[1])
    ]
    for load in load_e:
        load.start()

    barrier = pltpu.get_barrier_semaphore()

    def greet(to):
        pl.semaphore_signal(barrier, inc=1, device_id=to, device_id_type=MESH)

    for step in (4, 3, 5, 2, 6, 1, 7):
        to = lax.rem(half * 4 + z + step, 8)
        greet(device(to // 4, to % 4, y, x))
    for step in range(1, 16):
        to = lax.rem(plane + step, 16)
        greet(device(half, z, to % 4, to // 4))
    greet(device(half, z, y, x, 1 - core))

    pl.semaphore_wait(barrier, 23)

    def z_copy(m, distance, first, tiles):
        at = (lax.rem(x + distance, 4), pl.ds(first * TILE, tiles * TILE))
        return remote(b_own.at[at], b_far.at[at], z_send.at[m], z_recv.at[m], device(far, z, y, x))

    z_copies = [
        z_copy(2 * i + j, (2, 1, 3, 0)[i], *piece)
        for i in range(4)
        for j, piece in enumerate(HALVES if i < 3 else LAST)
    ]
    for m in range(HELD):
        if m % 2 == 0:
            loads[m // 2].wait()
        z_copies[m].start()
    loads[3].wait()

    @pl.when(core == 0)
    def _():
        for copy in z_copies[HELD:]:
            copy.start()

    load_a.wait()
    a_copy = remote(a_own, a_other, core_send, core_recv, device(half, z, y, x, 1 - core))
    a_copy.start()

    def prepare(source, which):
        def block_of(block, masked):
            at = block * BLK if masked else pl.multiple_of(block * BLK, BLK)
            for owner in range(4):
                lanes = pl.ds(at, EF - at if masked else BLK)
                if owner < 3:
                    part = source[pl.ds(owner * OWN, BLK), lanes]
                else:
                    part = pltpu.roll(source[pl.ds(ROWS - BLK, BLK), lanes], OWN, 0)
                if masked:
                    part = jnp.pad(part, ((0, 0), (0, KP - EF)))
                high, low = split(jnp.transpose(part))
                lanes = pl.ds(owner * WIDE + which * BLK, BLK)
                a_high[pl.ds(at, BLK), lanes] = high
                a_low[pl.ds(at, BLK), lanes] = low

        @pl.loop(0, KP // BLK - 1)
        def _(block):
            block_of(block, False)

        block_of(KP // BLK - 1, True)

    prepare(a_own, 0)
    for load in load_e:
        load.wait()
    denom_ref[...] = denominators(occ_ref[...].reshape(1, OCC), vir_ref[...].reshape(1, VIR), col, half, core * COLS + x * SLAB)
    a_copy.wait_recv()
    prepare(a_other, 1)

    def multiply(source, kind, m, distance, first, tiles):
        x_to = lax.rem(x + distance, 4)
        at = first * TILE
        if not isinstance(at, int):
            at = pl.multiple_of(at, TILE)
        cols = pl.ds(at, tiles * TILE)
        b = jnp.pad(source[x_to, cols, :], ((0, 0), (0, KP - EF)))
        b_high = b.astype(BF16).astype(F32)
        both = jnp.concatenate([b_high, b - b_high], axis=0).astype(BF16)
        for step in (2, 1, 3, 0):
            y_to = lax.rem(y + step, 4)
            lanes = pl.ds(pl.multiple_of(y_to * WIDE, WIDE), WIDE)
            upper = jnp.dot(both, a_high[:, lanes], preferred_element_type=F32)
            lower = jnp.dot(both, a_low[:, lanes], preferred_element_type=F32)
            n = tiles * TILE
            outgoing[kind, x_to, y_to, cols, :] = upper[:n] + (upper[n:] + (lower[:n] + lower[n:]))

            def send():
                remote(
                    outgoing.at[kind, x_to, y_to, cols], incoming.at[kind, plane, cols],
                    xy_send.at[m], xy_recv.at[m], device(half, z, y_to, x_to),
                ).start()

            if step:
                send()
            elif isinstance(distance, int):
                incoming[kind, plane, cols, :] = outgoing[kind, x_to, y_to, cols, :]
            else:

                @pl.when(distance == 0)
                def _():
                    incoming[kind, plane, cols, :] = outgoing[kind, x_to, y_to, cols, :]

                @pl.when(distance != 0)
                def _():
                    send()

    def xy_all(kind, m, tiles, count):
        blocks = (kind, pl.ds(0, count), pl.ds(0, tiles * TILE))
        return remote(incoming.at[blocks], incoming.at[blocks], xy_send.at[m], xy_recv.at[m], device(far, z, y, x))

    def end_copy(kind, which, cols):
        z_to = 2 * half + lax.rem(core + which, 2)
        half_to = far if kind else half
        return z_to, lambda: remote(
            reduced.at[kind, which, cols], landed.at[z, cols], end_send, end_recv, device(half_to, z_to, y, x)
        ).start()

    @pl.loop(0, 4)
    def _(i):
        multiply(b_own, 0, LOCAL + i, far_first(i), 0, 6)

    def finish_local():
        for i in range(4):
            xy_all(0, LOCAL + i, 6, 4 if i < 3 else 3).wait_recv()
        total = jnp.sum(incoming[0], axis=0)
        for which in range(2):
            reduced[0, which] = total[:, which * BLK : which * BLK + BLK]
        for which in range(2):
            z_to, send = end_copy(0, which, pl.ds(0, SLAB))

            @pl.when(z_to == z)
            def _():
                landed[z] = reduced[0, which]

            @pl.when(z_to != z)
            def _():
                send()

    @pl.loop(0, 7)
    def _(m):
        i = m // 2
        z_copy(m, far_first(i), 0, 3).wait_recv()
        @pl.when((core == 1) & (m == HELD - 1))
        def _():
            for copy in z_copies[HELD:]:
                copy.start()

        multiply(b_far, 1, m, far_first(i), 3 * lax.rem(m, 2), 3)

        @pl.when(m == 2)
        def _():
            finish_local()

    def slot(step):
        return lax.rem(x + step, 4) * 4

    for m in range(6):
        xy_all(1, m, 3, 4).wait_recv()
    total = jnp.sum(incoming[1, pl.ds(slot(1), 4)], axis=0)
    for step in (2, 3):
        total += jnp.sum(incoming[1, pl.ds(slot(step), 4)], axis=0)
    partial[...] = total

    def finish(j):
        first, tiles = LAST[j]
        cols = pl.ds(first * TILE, tiles * TILE)
        xy_all(1, 6 + j, tiles, 3).wait_recv()
        total = partial[cols, :] + jnp.sum(incoming[1, pl.ds(slot(0), 4), cols], axis=0)
        for which in range(2):
            reduced[1, which, cols, :] = total[:, which * BLK : which * BLK + BLK]
            end_copy(1, which, cols)[1]()

    for j in (1, 2):
        z_copies[6 + j].wait_recv()
        multiply(b_far, 1, 6 + j, 0, *LAST[j])
        if j == 1:
            finish(0)
    finish(1)
    finish(2)

    def end_all(count):
        blocks = landed.at[pl.ds(0, count)]
        return remote(blocks, blocks, end_send, end_recv, device(far, z, y, x))

    home = z // 2 == half

    @pl.when(home)
    def _():
        end_all(3).wait_recv()

    @pl.when(jnp.logical_not(home))
    def _():
        end_all(4).wait_recv()

    ladder_ref[...] = jnp.sum(landed[...], axis=0)

    a_copy.wait_send()
    for copy in z_copies:
        copy.wait_send()
    for m in range(PIECES):
        xy_all(1, m, 3 if m < 6 else LAST[m - 6][1], 4 if m < 6 else 3).wait_send()
    for i in range(4):
        xy_all(0, LOCAL + i, 6, 4 if i < 3 else 3).wait_send()
    end_all(3).wait_send()

    @pl.when(jnp.logical_not(home))
    def _():
        end_all(1).wait_send()


def shards(amplitudes, integrals, occ_energy, vir_energy):
    block = jax.ShapeDtypeStruct((SLAB, BLK), F32)
    dma = pltpu.SemaphoreType.DMA
    vmem = pl.BlockSpec(memory_space=pltpu.VMEM)
    hbm = pl.BlockSpec(memory_space=pltpu.HBM)
    ladder, denominator = pl.pallas_call(
        kernel,
        out_shape=(block, block),
        in_specs=[hbm] * 4,
        out_specs=(vmem, vmem),
        scratch_shapes=[
            pltpu.VMEM((ROWS, EF), F32),
            pltpu.VMEM((ROWS, EF), F32),
            pltpu.VMEM((KP, 4 * WIDE), BF16),
            pltpu.VMEM((KP, 4 * WIDE), BF16),
            pltpu.VMEM((4, SLAB, EF), F32),
            pltpu.VMEM((4, SLAB, EF), F32),
            pltpu.VMEM((2, 4, 4, SLAB, WIDE), F32),
            pltpu.VMEM((2, 16, SLAB, WIDE), F32),
            pltpu.VMEM((SLAB, WIDE), F32),
            pltpu.VMEM((2, 2, SLAB, BLK), F32),
            pltpu.VMEM((4, SLAB, BLK), F32),
            pltpu.VMEM((OCC,), F32),
            pltpu.VMEM((VIR,), F32),
            dma, dma((4,)), dma((2,)), dma, dma,
            dma((PIECES,)), dma((PIECES,)),
            dma((PIECES + 4,)), dma((PIECES + 4,)),
            dma, dma,
        ],
        compiler_params=pltpu.CompilerParams(collective_id=0, has_side_effects=True, vmem_limit_bytes=20 * 2**20),
    )(*[pltpu.with_memory_space_constraint(v, pltpu.HBM) for v in (amplitudes, integrals.T.reshape(4, SLAB, EF), occ_energy, vir_energy)])
    ladder = ladder[:, :OWN].T
    return ladder, ladder / denominator[:, :OWN].T


def solution(mesh):
    in_specs = (P("row", ("layer", "col")), P(("layer", "col"), "row"), P(), P())
    out_specs = (P("col", ("row", "layer")), P("col", ("row", "layer")))
    return jax.shard_map(shards, mesh=mesh, in_specs=in_specs, out_specs=out_specs, check_vma=False)
```

```python
import jax
import jax.numpy as jnp
from jax import lax
from jax.experimental import pallas as pl
from jax.experimental.pallas import tpu as pltpu
from jax.sharding import PartitionSpec as P

MESH = pl.DeviceIdType.MESH
F32, BF16 = jnp.float32, jnp.bfloat16

OCC, VIR = 64, 384
ROWS = 504
OWN = 126
EF = 1149
KP = 1152
COLS = 192
SLAB = 48
BLK = 128
TILE = 8
WIDE = 2 * BLK
HALVES = ((0, 3), (3, 3))
LAST = ((0, 3), (3, 2), (5, 1))
PIECES = 9
TAIL = slice(LAST[2][0] * TILE, SLAB)
HELD = 6
LOCAL = PIECES


def far_first(i):
    return jnp.where(i == 0, 2, jnp.where(i == 1, 1, jnp.where(i == 2, 3, 0)))


def split(value):
    high = value.astype(BF16)
    return high, (value - high.astype(F32)).astype(BF16)


def denominators(occ, vir, col, slab_a, slab_b):
    p = lax.broadcasted_iota(jnp.int32, (BLK, OCC), 0) + col * OWN
    i = lax.broadcasted_iota(jnp.int32, (BLK, OCC), 1)
    first = i * (2 * OCC - 1 - i) // 2
    is_i = (p >= first) & (p < first + OCC - 1 - i)
    j = p[:, :1] + jnp.sum(jnp.where(is_i, i + 1 - first, 0), axis=1, keepdims=True)
    row = lambda mask: jnp.sum(jnp.where(mask, occ, 0.0), axis=1, keepdims=True)
    pair_sum = row(is_i) + row(i == j)
    lane = lax.broadcasted_iota(jnp.int32, (1, VIR), 1)
    vir_a = jnp.sum(jnp.where(lane == slab_a, vir, 0.0), axis=1, keepdims=True)
    b = lax.broadcasted_iota(jnp.int32, (SLAB, VIR), 1)
    q = lax.broadcasted_iota(jnp.int32, (SLAB, VIR), 0) + slab_b
    vir_b = jnp.sum(jnp.where(b == q, vir, 0.0), axis=1, keepdims=True)
    return jnp.transpose(jnp.broadcast_to(pair_sum, (BLK, BLK)))[:SLAB] - (vir_a + vir_b)


def kernel(
    a_hbm, b_hbm, occ_hbm, vir_hbm, ladder_ref, denom_ref,
    a_own, a_other, a_high, a_low, b_own, b_far, outgoing, incoming, partial, reduced, landed, direct_in, occ_ref, vir_ref,
    a_sem, b_sem, e_sem, core_send, core_recv, z_send, z_recv, xy_send, xy_recv, end_send, end_recv, direct_send, direct_recv,
):
    row, col, x = lax.axis_index("row"), lax.axis_index("col"), lax.axis_index("layer")
    half, core = row // 2, row % 2
    z, y = col // 4, col % 4
    plane = x * 4 + y
    far = 1 - half

    def device(half_to, z_to, y_to, x_to, core_to=core):
        return (half_to * 2 + core_to, z_to * 4 + y_to, x_to)

    def remote(src, dst, send, recv, to):
        return pltpu.make_async_remote_copy(src, dst, send, recv, device_id=to, device_id_type=MESH)

    loads = []
    for i, distance in enumerate((2, 1, 3, 0)):
        owner = lax.rem(x + distance, 4)
        loads.append(pltpu.make_async_copy(b_hbm.at[owner], b_own.at[owner], b_sem.at[i]))
        loads[i].start()
    load_a = pltpu.make_async_copy(a_hbm, a_own, a_sem)
    load_a.start()
    load_e = [
        pltpu.make_async_copy(occ_hbm, occ_ref, e_sem.at[0]), pltpu.make_async_copy(vir_hbm, vir_ref, e_sem.at[1])
    ]
    for load in load_e:
        load.start()

    barrier = pltpu.get_barrier_semaphore()

    def greet(to):
        pl.semaphore_signal(barrier, inc=1, device_id=to, device_id_type=MESH)

    for step in (4, 3, 5, 2, 6, 1, 7):
        to = lax.rem(half * 4 + z + step, 8)
        greet(device(to // 4, to % 4, y, x))
    for step in range(1, 16):
        to = lax.rem(plane + step, 16)
        greet(device(half, z, to % 4, to // 4))
    greet(device(half, z, y, x, 1 - core))
    for y_step in range(1, 4):
        for step in range(1, 8):
            to = lax.rem(half * 4 + z + step, 8)
            greet(device(to // 4, to % 4, lax.rem(y + y_step, 4), x))

    pl.semaphore_wait(barrier, 44)

    def z_copy(m, distance, first, tiles):
        at = (lax.rem(x + distance, 4), pl.ds(first * TILE, tiles * TILE))
        return remote(b_own.at[at], b_far.at[at], z_send.at[m], z_recv.at[m], device(far, z, y, x))

    z_copies = [
        z_copy(2 * i + j, (2, 1, 3, 0)[i], *piece)
        for i in range(4)
        for j, piece in enumerate(HALVES if i < 3 else LAST)
    ]
    for m in range(HELD):
        if m % 2 == 0:
            loads[m // 2].wait()
        z_copies[m].start()
    loads[3].wait()

    @pl.when(core == 0)
    def _():
        for copy in z_copies[HELD:]:
            copy.start()

    load_a.wait()
    a_copy = remote(a_own, a_other, core_send, core_recv, device(half, z, y, x, 1 - core))
    a_copy.start()

    def prepare(source, which):
        def block_of(block, masked):
            at = block * BLK if masked else pl.multiple_of(block * BLK, BLK)
            for owner in range(4):
                lanes = pl.ds(at, EF - at if masked else BLK)
                if owner < 3:
                    part = source[pl.ds(owner * OWN, BLK), lanes]
                else:
                    part = pltpu.roll(source[pl.ds(ROWS - BLK, BLK), lanes], OWN, 0)
                if masked:
                    part = jnp.pad(part, ((0, 0), (0, KP - EF)))
                high, low = split(jnp.transpose(part))
                lanes = pl.ds(owner * WIDE + which * BLK, BLK)
                a_high[pl.ds(at, BLK), lanes] = high
                a_low[pl.ds(at, BLK), lanes] = low

        @pl.loop(0, KP // BLK - 1)
        def _(block):
            block_of(block, False)

        block_of(KP // BLK - 1, True)

    prepare(a_own, 0)
    for load in load_e:
        load.wait()
    denom_ref[...] = denominators(occ_ref[...].reshape(1, OCC), vir_ref[...].reshape(1, VIR), col, half, core * COLS + x * SLAB)
    a_copy.wait_recv()
    prepare(a_other, 1)

    def z_of(which):
        return 2 * half + lax.rem(core + which, 2)

    def multiply(source, kind, m, distance, first, tiles, direct=False):
        x_to = lax.rem(x + distance, 4)
        at = first * TILE
        if not isinstance(at, int):
            at = pl.multiple_of(at, TILE)
        cols = pl.ds(at, tiles * TILE)
        b = jnp.pad(source[x_to, cols, :], ((0, 0), (0, KP - EF)))
        b_high = b.astype(BF16).astype(F32)
        both = jnp.concatenate([b_high, b - b_high], axis=0).astype(BF16)
        for step in (2, 1, 3, 0):
            y_to = lax.rem(y + step, 4)
            lanes = pl.ds(pl.multiple_of(y_to * WIDE, WIDE), WIDE)
            upper = jnp.dot(both, a_high[:, lanes], preferred_element_type=F32)
            lower = jnp.dot(both, a_low[:, lanes], preferred_element_type=F32)
            n = tiles * TILE
            outgoing[kind, x_to, y_to, cols, :] = upper[:n] + (upper[n:] + (lower[:n] + lower[n:]))

            def send():
                remote(
                    outgoing.at[kind, x_to, y_to, cols], incoming.at[kind, plane, cols],
                    xy_send.at[m], xy_recv.at[m], device(half, z, y_to, x_to),
                ).start()

            if direct:
                for which in range(2):
                    remote(
                        outgoing.at[kind, x_to, y_to, cols, pl.ds(which * BLK, BLK)], direct_in.at[y * 4 + z],
                        direct_send, direct_recv, device(far, z_of(which), y_to, x),
                    ).start()
            elif step:
                send()
            elif isinstance(distance, int):
                incoming[kind, plane, cols, :] = outgoing[kind, x_to, y_to, cols, :]
            else:

                @pl.when(distance == 0)
                def _():
                    incoming[kind, plane, cols, :] = outgoing[kind, x_to, y_to, cols, :]

                @pl.when(distance != 0)
                def _():
                    send()

    def xy_all(kind, m, tiles, count):
        blocks = (kind, pl.ds(0, count), pl.ds(0, tiles * TILE))
        return remote(incoming.at[blocks], incoming.at[blocks], xy_send.at[m], xy_recv.at[m], device(far, z, y, x))

    def end_copy(kind, which, cols):
        z_to = z_of(which)
        half_to = far if kind else half
        return z_to, lambda: remote(
            reduced.at[kind, which, cols], landed.at[z, cols], end_send, end_recv, device(half_to, z_to, y, x)
        ).start()

    @pl.loop(0, 4)
    def _(i):
        multiply(b_own, 0, LOCAL + i, far_first(i), 0, 6)

    def finish_local():
        for i in range(4):
            xy_all(0, LOCAL + i, 6, 4 if i < 3 else 3).wait_recv()
        total = jnp.sum(incoming[0], axis=0)
        for which in range(2):
            reduced[0, which] = total[:, which * BLK : which * BLK + BLK]
        for which in range(2):
            z_to, send = end_copy(0, which, pl.ds(0, SLAB))

            @pl.when(z_to == z)
            def _():
                landed[z] = reduced[0, which]

            @pl.when(z_to != z)
            def _():
                send()

    @pl.loop(0, 7)
    def _(m):
        i = m // 2
        z_copy(m, far_first(i), 0, 3).wait_recv()
        @pl.when((core == 1) & (m == HELD - 1))
        def _():
            for copy in z_copies[HELD:]:
                copy.start()

        multiply(b_far, 1, m, far_first(i), 3 * lax.rem(m, 2), 3)

        @pl.when(m == 2)
        def _():
            finish_local()

    def slot(step):
        return lax.rem(x + step, 4) * 4

    for m in range(6):
        xy_all(1, m, 3, 4).wait_recv()
    total = jnp.sum(incoming[1, pl.ds(slot(1), 4)], axis=0)
    for step in (2, 3):
        total += jnp.sum(incoming[1, pl.ds(slot(step), 4)], axis=0)
    partial[...] = total

    def finish(j):
        first, tiles = LAST[j]
        cols = pl.ds(first * TILE, tiles * TILE)
        xy_all(1, 6 + j, tiles, 3).wait_recv()
        total = partial[cols, :] + jnp.sum(incoming[1, pl.ds(slot(0), 4), cols], axis=0)
        for which in range(2):
            lanes = slice(which * BLK, which * BLK + BLK)
            reduced[1, which, cols, :] = total[:, lanes]
            if j == 1:
                reduced[1, which, TAIL, :] = partial[TAIL, lanes]
        if j == 1:
            cols = pl.ds(first * TILE, SLAB - first * TILE)
        for which in range(2):
            end_copy(1, which, cols)[1]()

    for j in (1, 2):
        z_copies[6 + j].wait_recv()
        multiply(b_far, 1, 6 + j, 0, *LAST[j], direct=j == 2)
        if j == 1:
            finish(0)
    finish(1)

    def end_all(count):
        blocks = landed.at[pl.ds(0, count)]
        return remote(blocks, blocks, end_send, end_recv, device(far, z, y, x))

    def direct_all(count):
        blocks = direct_in.at[pl.ds(0, count)]
        return remote(blocks, blocks, direct_send, direct_recv, device(far, z, y, x))

    home = z // 2 == half

    @pl.when(home)
    def _():
        end_all(3).wait_recv()
        ladder_ref[...] = jnp.sum(landed[...], axis=0)

    @pl.when(jnp.logical_not(home))
    def _():
        end_all(4).wait_recv()
        ladder_ref[...] = jnp.sum(landed[...], axis=0)
        direct_all(16).wait_recv()
        ladder_ref[TAIL, :] += jnp.sum(direct_in[...], axis=0)

    a_copy.wait_send()
    for copy in z_copies:
        copy.wait_send()
    for m in range(PIECES - 1):
        xy_all(1, m, 3 if m < 6 else LAST[m - 6][1], 4 if m < 6 else 3).wait_send()
    direct_all(8).wait_send()
    for i in range(4):
        xy_all(0, LOCAL + i, 6, 4 if i < 3 else 3).wait_send()
    end_all(3).wait_send()

    @pl.when(jnp.logical_not(home))
    def _():
        end_all(1).wait_send()


def shards(amplitudes, integrals, occ_energy, vir_energy):
    block = jax.ShapeDtypeStruct((SLAB, BLK), F32)
    dma = pltpu.SemaphoreType.DMA
    vmem = pl.BlockSpec(memory_space=pltpu.VMEM)
    hbm = pl.BlockSpec(memory_space=pltpu.HBM)
    ladder, denominator = pl.pallas_call(
        kernel,
        out_shape=(block, block),
        in_specs=[hbm] * 4,
        out_specs=(vmem, vmem),
        scratch_shapes=[
            pltpu.VMEM((ROWS, EF), F32),
            pltpu.VMEM((ROWS, EF), F32),
            pltpu.VMEM((KP, 4 * WIDE), BF16),
            pltpu.VMEM((KP, 4 * WIDE), BF16),
            pltpu.VMEM((4, SLAB, EF), F32),
            pltpu.VMEM((4, SLAB, EF), F32),
            pltpu.VMEM((2, 4, 4, SLAB, WIDE), F32),
            pltpu.VMEM((2, 16, SLAB, WIDE), F32),
            pltpu.VMEM((SLAB, WIDE), F32),
            pltpu.VMEM((2, 2, SLAB, BLK), F32),
            pltpu.VMEM((4, SLAB, BLK), F32),
            pltpu.VMEM((16, TILE * LAST[2][1], BLK), F32),
            pltpu.VMEM((OCC,), F32),
            pltpu.VMEM((VIR,), F32),
            dma, dma((4,)), dma((2,)), dma, dma,
            dma((PIECES,)), dma((PIECES,)),
            dma((PIECES + 4,)), dma((PIECES + 4,)),
            dma, dma, dma, dma,
        ],
        compiler_params=pltpu.CompilerParams(collective_id=0, has_side_effects=True, vmem_limit_bytes=20 * 2**20),
    )(*[pltpu.with_memory_space_constraint(v, pltpu.HBM) for v in (amplitudes, integrals.T.reshape(4, SLAB, EF), occ_energy, vir_energy)])
    ladder = ladder[:, :OWN].T
    return ladder, ladder / denominator[:, :OWN].T


def solution(mesh):
    in_specs = (P("row", ("layer", "col")), P(("layer", "col"), "row"), P(), P())
    out_specs = (P("col", ("row", "layer")), P("col", ("row", "layer")))
    return jax.shard_map(shards, mesh=mesh, in_specs=in_specs, out_specs=out_specs, check_vma=False)
```

```python
import jax
import jax.numpy as jnp
from jax import lax
from jax.experimental import pallas as pl
from jax.experimental.pallas import tpu as pltpu
from jax.sharding import PartitionSpec as P

MESH = pl.DeviceIdType.MESH
F32, BF16 = jnp.float32, jnp.bfloat16

OCC, VIR = 64, 384
ROWS = 504
OWN = 126
EF = 1149
KP = 1152
COLS = 192
SLAB = 48
BLK = 128
TILE = 8
WIDE = 2 * BLK
HALVES = ((0, 3), (3, 3))
LAST = ((0, 3), (3, 2), (5, 1))
PIECES = 9
TAIL = slice(LAST[2][0] * TILE, SLAB)
HELD = 6
LOCAL = PIECES


def far_first(i):
    return jnp.where(i == 0, 2, jnp.where(i == 1, 1, jnp.where(i == 2, 3, 0)))


def split(value):
    high = value.astype(BF16)
    return high, (value - high.astype(F32)).astype(BF16)


def denominators(occ, vir, col, slab_a, slab_b):
    p = lax.broadcasted_iota(jnp.int32, (BLK, OCC), 0) + col * OWN
    i = lax.broadcasted_iota(jnp.int32, (BLK, OCC), 1)
    first = i * (2 * OCC - 1 - i) // 2
    is_i = (p >= first) & (p < first + OCC - 1 - i)
    j = p[:, :1] + jnp.sum(jnp.where(is_i, i + 1 - first, 0), axis=1, keepdims=True)
    row = lambda mask: jnp.sum(jnp.where(mask, occ, 0.0), axis=1, keepdims=True)
    pair_sum = row(is_i) + row(i == j)
    lane = lax.broadcasted_iota(jnp.int32, (1, VIR), 1)
    vir_a = jnp.sum(jnp.where(lane == slab_a, vir, 0.0), axis=1, keepdims=True)
    b = lax.broadcasted_iota(jnp.int32, (SLAB, VIR), 1)
    q = lax.broadcasted_iota(jnp.int32, (SLAB, VIR), 0) + slab_b
    vir_b = jnp.sum(jnp.where(b == q, vir, 0.0), axis=1, keepdims=True)
    return jnp.transpose(jnp.broadcast_to(pair_sum, (BLK, BLK)))[:SLAB] - (vir_a + vir_b)


def kernel(
    a_hbm, b_hbm, occ_hbm, vir_hbm, ladder_ref, denom_ref,
    a_own, a_other, a_high, a_low, b_own, b_far, outgoing, incoming, partial, reduced, landed, direct_in, occ_ref, vir_ref,
    a_sem, b_sem, e_sem, core_send, core_recv, z_send, z_recv, xy_send, xy_recv, end_send, end_recv, direct_send, direct_recv,
):
    row, col, x = lax.axis_index("row"), lax.axis_index("col"), lax.axis_index("layer")
    half, core = row // 2, row % 2
    z, y = col // 4, col % 4
    plane = x * 4 + y
    far = 1 - half

    def device(half_to, z_to, y_to, x_to, core_to=core):
        return (half_to * 2 + core_to, z_to * 4 + y_to, x_to)

    def remote(src, dst, send, recv, to):
        return pltpu.make_async_remote_copy(src, dst, send, recv, device_id=to, device_id_type=MESH)

    barrier = pltpu.get_barrier_semaphore()

    def greet(to):
        pl.semaphore_signal(barrier, inc=1, device_id=to, device_id_type=MESH)

    for step in (4, 3, 5, 2, 6, 1, 7):
        to = lax.rem(half * 4 + z + step, 8)
        greet(device(to // 4, to % 4, y, x))
    for step in range(1, 16):
        to = lax.rem(plane + step, 16)
        greet(device(half, z, to % 4, to // 4))
    greet(device(half, z, y, x, 1 - core))
    for y_step in range(1, 4):
        for step in range(1, 8):
            to = lax.rem(half * 4 + z + step, 8)
            greet(device(to // 4, to % 4, lax.rem(y + y_step, 4), x))

    loads = []
    for i, distance in enumerate((2, 1, 3, 0)):
        owner = lax.rem(x + distance, 4)
        loads.append(pltpu.make_async_copy(b_hbm.at[owner], b_own.at[owner], b_sem.at[i]))
        loads[i].start()
    load_a = pltpu.make_async_copy(a_hbm, a_own, a_sem)
    load_a.start()
    load_e = [
        pltpu.make_async_copy(occ_hbm, occ_ref, e_sem.at[0]), pltpu.make_async_copy(vir_hbm, vir_ref, e_sem.at[1])
    ]
    for load in load_e:
        load.start()

    pl.semaphore_wait(barrier, 44)

    def z_copy(m, distance, first, tiles):
        at = (lax.rem(x + distance, 4), pl.ds(first * TILE, tiles * TILE))
        return remote(b_own.at[at], b_far.at[at], z_send.at[m], z_recv.at[m], device(far, z, y, x))

    z_copies = [
        z_copy(2 * i + j, (2, 1, 3, 0)[i], *piece)
        for i in range(4)
        for j, piece in enumerate(HALVES if i < 3 else LAST)
    ]
    for m in range(HELD):
        if m % 2 == 0:
            loads[m // 2].wait()
        z_copies[m].start()
    loads[3].wait()

    @pl.when(core == 0)
    def _():
        for copy in z_copies[HELD:]:
            copy.start()

    load_a.wait()
    a_copy = remote(a_own, a_other, core_send, core_recv, device(half, z, y, x, 1 - core))
    a_copy.start()

    def prepare(source, which):
        def block_of(block, masked):
            at = block * BLK if masked else pl.multiple_of(block * BLK, BLK)
            for owner in range(4):
                lanes = pl.ds(at, EF - at if masked else BLK)
                if owner < 3:
                    part = source[pl.ds(owner * OWN, BLK), lanes]
                else:
                    part = pltpu.roll(source[pl.ds(ROWS - BLK, BLK), lanes], OWN, 0)
                if masked:
                    part = jnp.pad(part, ((0, 0), (0, KP - EF)))
                high, low = split(jnp.transpose(part))
                lanes = pl.ds(owner * WIDE + which * BLK, BLK)
                a_high[pl.ds(at, BLK), lanes] = high
                a_low[pl.ds(at, BLK), lanes] = low

        @pl.loop(0, KP // BLK - 1)
        def _(block):
            block_of(block, False)

        block_of(KP // BLK - 1, True)

    prepare(a_own, 0)
    for load in load_e:
        load.wait()
    denom_ref[...] = denominators(occ_ref[...].reshape(1, OCC), vir_ref[...].reshape(1, VIR), col, half, core * COLS + x * SLAB)
    a_copy.wait_recv()
    prepare(a_other, 1)

    def z_of(which):
        return 2 * half + lax.rem(core + which, 2)

    def multiply(source, kind, m, distance, first, tiles, direct=False):
        x_to = lax.rem(x + distance, 4)
        at = first * TILE
        if not isinstance(at, int):
            at = pl.multiple_of(at, TILE)
        cols = pl.ds(at, tiles * TILE)
        b = jnp.pad(source[x_to, cols, :], ((0, 0), (0, KP - EF)))
        b_high = b.astype(BF16).astype(F32)
        both = jnp.concatenate([b_high, b - b_high], axis=0).astype(BF16)
        for step in (2, 1, 3, 0):
            y_to = lax.rem(y + step, 4)
            lanes = pl.ds(pl.multiple_of(y_to * WIDE, WIDE), WIDE)
            upper = jnp.dot(both, a_high[:, lanes], preferred_element_type=F32)
            lower = jnp.dot(both, a_low[:, lanes], preferred_element_type=F32)
            n = tiles * TILE
            outgoing[kind, x_to, y_to, cols, :] = upper[:n] + (upper[n:] + (lower[:n] + lower[n:]))

            def send():
                remote(
                    outgoing.at[kind, x_to, y_to, cols], incoming.at[kind, plane, cols],
                    xy_send.at[m], xy_recv.at[m], device(half, z, y_to, x_to),
                ).start()

            if direct:
                for which in range(2):
                    remote(
                        outgoing.at[kind, x_to, y_to, cols, pl.ds(which * BLK, BLK)], direct_in.at[y * 4 + z],
                        direct_send, direct_recv, device(far, z_of(which), y_to, x),
                    ).start()
            elif step:
                send()
            elif isinstance(distance, int):
                incoming[kind, plane, cols, :] = outgoing[kind, x_to, y_to, cols, :]
            else:

                @pl.when(distance == 0)
                def _():
                    incoming[kind, plane, cols, :] = outgoing[kind, x_to, y_to, cols, :]

                @pl.when(distance != 0)
                def _():
                    send()

    def xy_all(kind, m, tiles, count):
        blocks = (kind, pl.ds(0, count), pl.ds(0, tiles * TILE))
        return remote(incoming.at[blocks], incoming.at[blocks], xy_send.at[m], xy_recv.at[m], device(far, z, y, x))

    def end_copy(kind, which, cols):
        z_to = z_of(which)
        half_to = far if kind else half
        return z_to, lambda: remote(
            reduced.at[kind, which, cols], landed.at[z, cols], end_send, end_recv, device(half_to, z_to, y, x)
        ).start()

    @pl.loop(0, 4)
    def _(i):
        multiply(b_own, 0, LOCAL + i, far_first(i), 0, 6)

    def finish_local():
        for i in range(4):
            xy_all(0, LOCAL + i, 6, 4 if i < 3 else 3).wait_recv()
        total = jnp.sum(incoming[0], axis=0)
        for which in range(2):
            reduced[0, which] = total[:, which * BLK : which * BLK + BLK]
        for which in range(2):
            z_to, send = end_copy(0, which, pl.ds(0, SLAB))

            @pl.when(z_to == z)
            def _():
                landed[z] = reduced[0, which]

            @pl.when(z_to != z)
            def _():
                send()

    @pl.loop(0, 7)
    def _(m):
        i = m // 2
        z_copy(m, far_first(i), 0, 3).wait_recv()
        @pl.when((core == 1) & (m == HELD - 1))
        def _():
            for copy in z_copies[HELD:]:
                copy.start()

        multiply(b_far, 1, m, far_first(i), 3 * lax.rem(m, 2), 3)

        @pl.when(m == 2)
        def _():
            finish_local()

    def slot(step):
        return lax.rem(x + step, 4) * 4

    for m in range(6):
        xy_all(1, m, 3, 4).wait_recv()
    total = jnp.sum(incoming[1, pl.ds(slot(1), 4)], axis=0)
    for step in (2, 3):
        total += jnp.sum(incoming[1, pl.ds(slot(step), 4)], axis=0)
    partial[...] = total

    def finish(j):
        first, tiles = LAST[j]
        cols = pl.ds(first * TILE, tiles * TILE)
        xy_all(1, 6 + j, tiles, 3).wait_recv()
        total = partial[cols, :] + jnp.sum(incoming[1, pl.ds(slot(0), 4), cols], axis=0)
        for which in range(2):
            lanes = slice(which * BLK, which * BLK + BLK)
            reduced[1, which, cols, :] = total[:, lanes]
            if j == 1:
                reduced[1, which, TAIL, :] = partial[TAIL, lanes]
        if j == 1:
            cols = pl.ds(first * TILE, SLAB - first * TILE)
        for which in range(2):
            end_copy(1, which, cols)[1]()

    for j in (1, 2):
        z_copies[6 + j].wait_recv()
        multiply(b_far, 1, 6 + j, 0, *LAST[j], direct=j == 2)
        if j == 1:
            finish(0)
    finish(1)

    def end_all(count):
        blocks = landed.at[pl.ds(0, count)]
        return remote(blocks, blocks, end_send, end_recv, device(far, z, y, x))

    def direct_all(count):
        blocks = direct_in.at[pl.ds(0, count)]
        return remote(blocks, blocks, direct_send, direct_recv, device(far, z, y, x))

    home = z // 2 == half

    @pl.when(home)
    def _():
        end_all(3).wait_recv()
        ladder_ref[...] = jnp.sum(landed[...], axis=0)

    @pl.when(jnp.logical_not(home))
    def _():
        end_all(4).wait_recv()
        ladder_ref[...] = jnp.sum(landed[...], axis=0)
        direct_all(16).wait_recv()
        ladder_ref[TAIL, :] += jnp.sum(direct_in[...], axis=0)

    a_copy.wait_send()
    for copy in z_copies:
        copy.wait_send()
    for m in range(PIECES - 1):
        xy_all(1, m, 3 if m < 6 else LAST[m - 6][1], 4 if m < 6 else 3).wait_send()
    direct_all(8).wait_send()
    for i in range(4):
        xy_all(0, LOCAL + i, 6, 4 if i < 3 else 3).wait_send()
    end_all(3).wait_send()

    @pl.when(jnp.logical_not(home))
    def _():
        end_all(1).wait_send()


def shards(amplitudes, integrals, occ_energy, vir_energy):
    block = jax.ShapeDtypeStruct((SLAB, BLK), F32)
    dma = pltpu.SemaphoreType.DMA
    vmem = pl.BlockSpec(memory_space=pltpu.VMEM)
    hbm = pl.BlockSpec(memory_space=pltpu.HBM)
    ladder, denominator = pl.pallas_call(
        kernel,
        out_shape=(block, block),
        in_specs=[hbm] * 4,
        out_specs=(vmem, vmem),
        scratch_shapes=[
            pltpu.VMEM((ROWS, EF), F32),
            pltpu.VMEM((ROWS, EF), F32),
            pltpu.VMEM((KP, 4 * WIDE), BF16),
            pltpu.VMEM((KP, 4 * WIDE), BF16),
            pltpu.VMEM((4, SLAB, EF), F32),
            pltpu.VMEM((4, SLAB, EF), F32),
            pltpu.VMEM((2, 4, 4, SLAB, WIDE), F32),
            pltpu.VMEM((2, 16, SLAB, WIDE), F32),
            pltpu.VMEM((SLAB, WIDE), F32),
            pltpu.VMEM((2, 2, SLAB, BLK), F32),
            pltpu.VMEM((4, SLAB, BLK), F32),
            pltpu.VMEM((16, TILE * LAST[2][1], BLK), F32),
            pltpu.VMEM((OCC,), F32),
            pltpu.VMEM((VIR,), F32),
            dma, dma((4,)), dma((2,)), dma, dma,
            dma((PIECES,)), dma((PIECES,)),
            dma((PIECES + 4,)), dma((PIECES + 4,)),
            dma, dma, dma, dma,
        ],
        compiler_params=pltpu.CompilerParams(collective_id=0, has_side_effects=True, vmem_limit_bytes=20 * 2**20),
    )(*[pltpu.with_memory_space_constraint(v, pltpu.HBM) for v in (amplitudes, integrals.T.reshape(4, SLAB, EF), occ_energy, vir_energy)])
    ladder = ladder[:, :OWN].T
    return ladder, ladder / denominator[:, :OWN].T


def solution(mesh):
    in_specs = (P("row", ("layer", "col")), P(("layer", "col"), "row"), P(), P())
    out_specs = (P("col", ("row", "layer")), P("col", ("row", "layer")))
    return jax.shard_map(shards, mesh=mesh, in_specs=in_specs, out_specs=out_specs, check_vma=False)
```

```python
import jax
import jax.numpy as jnp
from jax import lax
from jax.experimental import pallas as pl
from jax.experimental.pallas import tpu as pltpu
from jax.sharding import PartitionSpec as P

MESH = pl.DeviceIdType.MESH
F32, BF16 = jnp.float32, jnp.bfloat16

OCC, VIR = 64, 384
ROWS = 504
OWN = 126
EF = 1149
KP = 1152
COLS = 192
SLAB = 48
BLK = 128
TILE = 8
WIDE = 2 * BLK
HALVES = ((0, 3), (3, 3))
LAST = ((0, 3), (3, 2), (5, 1))
PIECES = 9
TAIL = slice(LAST[2][0] * TILE, SLAB)
HELD = 6
LOCAL = PIECES


def far_first(i):
    return jnp.where(i == 0, 2, jnp.where(i == 1, 1, jnp.where(i == 2, 3, 0)))


def split(value):
    high = value.astype(BF16)
    return high, (value - high.astype(F32)).astype(BF16)


def denominators(occ, vir, col, slab_a, slab_b):
    p = lax.broadcasted_iota(jnp.int32, (BLK, OCC), 0) + col * OWN
    i = lax.broadcasted_iota(jnp.int32, (BLK, OCC), 1)
    first = i * (2 * OCC - 1 - i) // 2
    is_i = (p >= first) & (p < first + OCC - 1 - i)
    j = p[:, :1] + jnp.sum(jnp.where(is_i, i + 1 - first, 0), axis=1, keepdims=True)
    row = lambda mask: jnp.sum(jnp.where(mask, occ, 0.0), axis=1, keepdims=True)
    pair_sum = row(is_i) + row(i == j)
    lane = lax.broadcasted_iota(jnp.int32, (1, VIR), 1)
    vir_a = jnp.sum(jnp.where(lane == slab_a, vir, 0.0), axis=1, keepdims=True)
    b = lax.broadcasted_iota(jnp.int32, (SLAB, VIR), 1)
    q = lax.broadcasted_iota(jnp.int32, (SLAB, VIR), 0) + slab_b
    vir_b = jnp.sum(jnp.where(b == q, vir, 0.0), axis=1, keepdims=True)
    return jnp.transpose(jnp.broadcast_to(pair_sum, (BLK, BLK)))[:SLAB] - (vir_a + vir_b)


def kernel(
    a_hbm, b_hbm, occ_hbm, vir_hbm, ladder_ref, denom_ref,
    a_own, a_other, a_high, a_low, b_own, b_far, outgoing, incoming, partial, reduced, landed, direct_in, occ_ref, vir_ref,
    a_sem, b_sem, e_sem, core_send, core_recv, z_send, z_recv, xy_send, xy_recv, end_send, end_recv, direct_send, direct_recv,
):
    row, col, x = lax.axis_index("row"), lax.axis_index("col"), lax.axis_index("layer")
    half, core = row // 2, row % 2
    z, y = col // 4, col % 4
    plane = x * 4 + y
    far = 1 - half

    def device(half_to, z_to, y_to, x_to, core_to=core):
        return (half_to * 2 + core_to, z_to * 4 + y_to, x_to)

    def remote(src, dst, send, recv, to):
        return pltpu.make_async_remote_copy(src, dst, send, recv, device_id=to, device_id_type=MESH)

    loads = []
    for i, distance in enumerate((2, 1, 3, 0)):
        owner = lax.rem(x + distance, 4)
        loads.append(pltpu.make_async_copy(b_hbm.at[owner], b_own.at[owner], b_sem.at[i]))
        loads[i].start()
    load_a = pltpu.make_async_copy(a_hbm, a_own, a_sem)
    load_a.start()
    load_e = [
        pltpu.make_async_copy(occ_hbm, occ_ref, e_sem.at[0]), pltpu.make_async_copy(vir_hbm, vir_ref, e_sem.at[1])
    ]
    for load in load_e:
        load.start()

    barrier = pltpu.get_barrier_semaphore()

    def greet(to):
        pl.semaphore_signal(barrier, inc=1, device_id=to, device_id_type=MESH)

    for step in (4, 3, 5, 2, 6, 1, 7):
        to = lax.rem(half * 4 + z + step, 8)
        greet(device(to // 4, to % 4, y, x))
    for step in range(1, 16):
        to = lax.rem(plane + step, 16)
        greet(device(half, z, to % 4, to // 4))
    greet(device(half, z, y, x, 1 - core))
    for y_step in range(1, 4):
        for step in range(1, 8):
            to = lax.rem(half * 4 + z + step, 8)
            greet(device(to // 4, to % 4, lax.rem(y + y_step, 4), x))

    pl.semaphore_wait(barrier, 44)

    def z_copy(m, distance, first, tiles):
        at = (lax.rem(x + distance, 4), pl.ds(first * TILE, tiles * TILE))
        return remote(b_own.at[at], b_far.at[at], z_send.at[m], z_recv.at[m], device(far, z, y, x))

    z_copies = [
        z_copy(2 * i + j, (2, 1, 3, 0)[i], *piece)
        for i in range(4)
        for j, piece in enumerate(HALVES if i < 3 else LAST)
    ]
    for m in range(HELD):
        if m % 2 == 0:
            loads[m // 2].wait()
        z_copies[m].start()
    loads[3].wait()

    @pl.when(core == 0)
    def _():
        for copy in z_copies[HELD:]:
            copy.start()

    load_a.wait()
    a_copy = remote(a_own, a_other, core_send, core_recv, device(half, z, y, x, 1 - core))
    a_copy.start()

    def prepare(source, which):
        def block_of(block, masked):
            at = block * BLK if masked else pl.multiple_of(block * BLK, BLK)
            for owner in range(4):
                lanes = pl.ds(at, EF - at if masked else BLK)
                if owner < 3:
                    part = source[pl.ds(owner * OWN, BLK), lanes]
                else:
                    part = pltpu.roll(source[pl.ds(ROWS - BLK, BLK), lanes], OWN, 0)
                if masked:
                    part = jnp.pad(part, ((0, 0), (0, KP - EF)))
                high, low = split(jnp.transpose(part))
                lanes = pl.ds(owner * WIDE + which * BLK, BLK)
                a_high[pl.ds(at, BLK), lanes] = high
                a_low[pl.ds(at, BLK), lanes] = low

        @pl.loop(0, KP // BLK - 1)
        def _(block):
            block_of(block, False)

        block_of(KP // BLK - 1, True)

    prepare(a_own, 0)
    for load in load_e:
        load.wait()
    denom_ref[...] = denominators(occ_ref[...].reshape(1, OCC), vir_ref[...].reshape(1, VIR), col, half, core * COLS + x * SLAB)
    a_copy.wait_recv()
    prepare(a_other, 1)

    def z_of(which):
        return 2 * half + lax.rem(core + which, 2)

    def multiply(source, kind, m, distance, first, tiles, direct=False):
        x_to = lax.rem(x + distance, 4)
        at = first * TILE
        if not isinstance(at, int):
            at = pl.multiple_of(at, TILE)
        cols = pl.ds(at, tiles * TILE)
        b = jnp.pad(source[x_to, cols, :], ((0, 0), (0, KP - EF)))
        b_high = b.astype(BF16).astype(F32)
        both = jnp.concatenate([b_high, b - b_high], axis=0).astype(BF16)
        for step in (2, 1, 3, 0):
            y_to = lax.rem(y + step, 4)
            lanes = pl.ds(pl.multiple_of(y_to * WIDE, WIDE), WIDE)
            upper = jnp.dot(both, a_high[:, lanes], preferred_element_type=F32)
            lower = jnp.dot(both, a_low[:, lanes], preferred_element_type=F32)
            n = tiles * TILE
            outgoing[kind, x_to, y_to, cols, :] = upper[:n] + (upper[n:] + (lower[:n] + lower[n:]))

            def send():
                remote(
                    outgoing.at[kind, x_to, y_to, cols], incoming.at[kind, plane, cols],
                    xy_send.at[m], xy_recv.at[m], device(half, z, y_to, x_to),
                ).start()

            if direct:
                for which in range(2):
                    remote(
                        outgoing.at[kind, x_to, y_to, cols, pl.ds(which * BLK, BLK)], direct_in.at[y * 4 + z],
                        direct_send, direct_recv, device(far, z_of(which), y_to, x),
                    ).start()
            elif step:
                send()
            elif isinstance(distance, int):
                incoming[kind, plane, cols, :] = outgoing[kind, x_to, y_to, cols, :]
            else:

                @pl.when(distance == 0)
                def _():
                    incoming[kind, plane, cols, :] = outgoing[kind, x_to, y_to, cols, :]

                @pl.when(distance != 0)
                def _():
                    send()

    def xy_all(kind, m, tiles, count):
        blocks = (kind, pl.ds(0, count), pl.ds(0, tiles * TILE))
        return remote(incoming.at[blocks], incoming.at[blocks], xy_send.at[m], xy_recv.at[m], device(far, z, y, x))

    def end_copy(kind, which, cols):
        z_to = z_of(which)
        half_to = far if kind else half
        return z_to, lambda: remote(
            reduced.at[kind, which, cols], landed.at[z, cols], end_send, end_recv, device(half_to, z_to, y, x)
        ).start()

    @pl.loop(0, 4)
    def _(i):
        multiply(b_own, 0, LOCAL + i, far_first(i), 0, 6)

    def finish_local():
        for i in range(4):
            xy_all(0, LOCAL + i, 6, 4 if i < 3 else 3).wait_recv()
        total = jnp.sum(incoming[0], axis=0)
        for which in range(2):
            reduced[0, which] = total[:, which * BLK : which * BLK + BLK]
        for which in range(2):
            z_to, send = end_copy(0, which, pl.ds(0, SLAB))

            @pl.when(z_to == z)
            def _():
                landed[z] = reduced[0, which]

            @pl.when(z_to != z)
            def _():
                send()

    @pl.loop(0, 7)
    def _(m):
        i = m // 2
        z_copy(m, far_first(i), 0, 3).wait_recv()
        @pl.when((core == 1) & (m == HELD - 1))
        def _():
            for copy in z_copies[HELD:]:
                copy.start()

        multiply(b_far, 1, m, far_first(i), 3 * lax.rem(m, 2), 3)

        @pl.when(m == 2)
        def _():
            finish_local()

    def slot(step):
        return lax.rem(x + step, 4) * 4

    for m in range(6):
        xy_all(1, m, 3, 4).wait_recv()
    total = jnp.sum(incoming[1, pl.ds(slot(1), 4)], axis=0)
    for step in (2, 3):
        total += jnp.sum(incoming[1, pl.ds(slot(step), 4)], axis=0)
    partial[...] = total

    def finish(j):
        first, tiles = LAST[j]
        cols = pl.ds(first * TILE, tiles * TILE)
        xy_all(1, 6 + j, tiles, 3).wait_recv()
        total = partial[cols, :] + jnp.sum(incoming[1, pl.ds(slot(0), 4), cols], axis=0)
        for which in range(2):
            lanes = slice(which * BLK, which * BLK + BLK)
            reduced[1, which, cols, :] = total[:, lanes]
            if j == 1:
                reduced[1, which, TAIL, :] = partial[TAIL, lanes]
        if j == 1:
            cols = pl.ds(first * TILE, SLAB - first * TILE)
        for which in range(2):
            end_copy(1, which, cols)[1]()

    for j in (1, 2):
        z_copies[6 + j].wait_recv()
        multiply(b_far, 1, 6 + j, 0, *LAST[j], direct=j == 2)
        if j == 1:
            finish(0)
    finish(1)

    def end_all(count):
        blocks = landed.at[pl.ds(0, count)]
        return remote(blocks, blocks, end_send, end_recv, device(far, z, y, x))

    def direct_all(count):
        blocks = direct_in.at[pl.ds(0, count)]
        return remote(blocks, blocks, direct_send, direct_recv, device(far, z, y, x))

    a_copy.wait_send()
    for copy in z_copies:
        copy.wait_send()
    for m in range(PIECES - 1):
        xy_all(1, m, 3 if m < 6 else LAST[m - 6][1], 4 if m < 6 else 3).wait_send()
    for i in range(4):
        xy_all(0, LOCAL + i, 6, 4 if i < 3 else 3).wait_send()

    home = z // 2 == half

    @pl.when(home)
    def _():
        end_all(3).wait_recv()
        ladder_ref[...] = jnp.sum(landed[...], axis=0)

    @pl.when(jnp.logical_not(home))
    def _():
        end_all(4).wait_recv()
        ladder_ref[...] = jnp.sum(landed[...], axis=0)
        direct_all(16).wait_recv()
        ladder_ref[TAIL, :] += jnp.sum(direct_in[...], axis=0)

    direct_all(8).wait_send()
    end_all(3).wait_send()

    @pl.when(jnp.logical_not(home))
    def _():
        end_all(1).wait_send()


def shards(amplitudes, integrals, occ_energy, vir_energy):
    block = jax.ShapeDtypeStruct((SLAB, BLK), F32)
    dma = pltpu.SemaphoreType.DMA
    vmem = pl.BlockSpec(memory_space=pltpu.VMEM)
    hbm = pl.BlockSpec(memory_space=pltpu.HBM)
    ladder, denominator = pl.pallas_call(
        kernel,
        out_shape=(block, block),
        in_specs=[hbm] * 4,
        out_specs=(vmem, vmem),
        scratch_shapes=[
            pltpu.VMEM((ROWS, EF), F32),
            pltpu.VMEM((ROWS, EF), F32),
            pltpu.VMEM((KP, 4 * WIDE), BF16),
            pltpu.VMEM((KP, 4 * WIDE), BF16),
            pltpu.VMEM((4, SLAB, EF), F32),
            pltpu.VMEM((4, SLAB, EF), F32),
            pltpu.VMEM((2, 4, 4, SLAB, WIDE), F32),
            pltpu.VMEM((2, 16, SLAB, WIDE), F32),
            pltpu.VMEM((SLAB, WIDE), F32),
            pltpu.VMEM((2, 2, SLAB, BLK), F32),
            pltpu.VMEM((4, SLAB, BLK), F32),
            pltpu.VMEM((16, TILE * LAST[2][1], BLK), F32),
            pltpu.VMEM((OCC,), F32),
            pltpu.VMEM((VIR,), F32),
            dma, dma((4,)), dma((2,)), dma, dma,
            dma((PIECES,)), dma((PIECES,)),
            dma((PIECES + 4,)), dma((PIECES + 4,)),
            dma, dma, dma, dma,
        ],
        compiler_params=pltpu.CompilerParams(collective_id=0, has_side_effects=True, vmem_limit_bytes=20 * 2**20),
    )(*[pltpu.with_memory_space_constraint(v, pltpu.HBM) for v in (amplitudes, integrals.T.reshape(4, SLAB, EF), occ_energy, vir_energy)])
    ladder = ladder[:, :OWN].T
    return ladder, ladder / denominator[:, :OWN].T


def solution(mesh):
    in_specs = (P("row", ("layer", "col")), P(("layer", "col"), "row"), P(), P())
    out_specs = (P("col", ("row", "layer")), P("col", ("row", "layer")))
    return jax.shard_map(shards, mesh=mesh, in_specs=in_specs, out_specs=out_specs, check_vma=False)
```

```python
import jax
import jax.numpy as jnp
from jax import lax
from jax.experimental import pallas as pl
from jax.experimental.pallas import tpu as pltpu
from jax.sharding import PartitionSpec as P

MESH = pl.DeviceIdType.MESH
F32, BF16 = jnp.float32, jnp.bfloat16

OCC, VIR = 64, 384
ROWS = 504
OWN = 126
EF = 1149
KP = 1152
COLS = 192
SLAB = 48
BLK = 128
TILE = 8
WIDE = 2 * BLK
HALVES = ((0, 3), (3, 3))
LAST = ((0, 3), (3, 2), (5, 1))
PIECES = 9
TAIL = slice(LAST[2][0] * TILE, SLAB)
HELD = 6
LOCAL = PIECES


def far_first(i):
    return jnp.where(i == 0, 2, jnp.where(i == 1, 1, jnp.where(i == 2, 3, 0)))


def split(value):
    high = value.astype(BF16)
    return high, (value - high.astype(F32)).astype(BF16)


def denominators(occ, vir, col, slab_a, slab_b):
    p = lax.broadcasted_iota(jnp.int32, (BLK, OCC), 0) + col * OWN
    i = lax.broadcasted_iota(jnp.int32, (BLK, OCC), 1)
    first = i * (2 * OCC - 1 - i) // 2
    is_i = (p >= first) & (p < first + OCC - 1 - i)
    j = p[:, :1] + jnp.sum(jnp.where(is_i, i + 1 - first, 0), axis=1, keepdims=True)
    row = lambda mask: jnp.sum(jnp.where(mask, occ, 0.0), axis=1, keepdims=True)
    pair_sum = row(is_i) + row(i == j)
    lane = lax.broadcasted_iota(jnp.int32, (1, VIR), 1)
    vir_a = jnp.sum(jnp.where(lane == slab_a, vir, 0.0), axis=1, keepdims=True)
    b = lax.broadcasted_iota(jnp.int32, (SLAB, VIR), 1)
    q = lax.broadcasted_iota(jnp.int32, (SLAB, VIR), 0) + slab_b
    vir_b = jnp.sum(jnp.where(b == q, vir, 0.0), axis=1, keepdims=True)
    return jnp.transpose(jnp.broadcast_to(pair_sum, (BLK, BLK)))[:SLAB] - (vir_a + vir_b)


def kernel(
    a_hbm, b_hbm, occ_hbm, vir_hbm, ladder_ref, denom_ref,
    a_own, a_other, a_high, a_low, b_own, b_far, outgoing, incoming, partial, reduced, landed, direct_in, occ_ref, vir_ref,
    a_sem, b_sem, e_sem, core_send, core_recv, z_send, z_recv, xy_send, xy_recv, end_send, end_recv, direct_send, direct_recv,
):
    row, col, x = lax.axis_index("row"), lax.axis_index("col"), lax.axis_index("layer")
    half, core = row // 2, row % 2
    z, y = col // 4, col % 4
    plane = x * 4 + y
    far = 1 - half

    def device(half_to, z_to, y_to, x_to, core_to=core):
        return (half_to * 2 + core_to, z_to * 4 + y_to, x_to)

    def remote(src, dst, send, recv, to):
        return pltpu.make_async_remote_copy(src, dst, send, recv, device_id=to, device_id_type=MESH)

    loads = []
    for i, distance in enumerate((2, 1, 3, 0)):
        owner = lax.rem(x + distance, 4)
        loads.append(pltpu.make_async_copy(b_hbm.at[owner], b_own.at[owner], b_sem.at[i]))
        loads[i].start()
    load_a = pltpu.make_async_copy(a_hbm, a_own, a_sem)
    load_a.start()
    load_e = [
        pltpu.make_async_copy(occ_hbm, occ_ref, e_sem.at[0]), pltpu.make_async_copy(vir_hbm, vir_ref, e_sem.at[1])
    ]
    for load in load_e:
        load.start()

    barrier = pltpu.get_barrier_semaphore()

    def greet(to):
        pl.semaphore_signal(barrier, inc=1, device_id=to, device_id_type=MESH)

    for step in (4, 3, 5, 2, 6, 1, 7):
        to = lax.rem(half * 4 + z + step, 8)
        greet(device(to // 4, to % 4, y, x))
    for step in range(1, 16):
        to = lax.rem(plane + step, 16)
        greet(device(half, z, to % 4, to // 4))
    greet(device(half, z, y, x, 1 - core))
    for y_step in range(1, 4):
        for step in range(1, 8):
            to = lax.rem(half * 4 + z + step, 8)
            greet(device(to // 4, to % 4, lax.rem(y + y_step, 4), x))

    pl.semaphore_wait(barrier, 44)

    def z_copy(m, distance, first, tiles):
        at = (lax.rem(x + distance, 4), pl.ds(first * TILE, tiles * TILE))
        return remote(b_own.at[at], b_far.at[at], z_send.at[m], z_recv.at[m], device(far, z, y, x))

    z_copies = [
        z_copy(2 * i + j, (2, 1, 3, 0)[i], *piece)
        for i in range(4)
        for j, piece in enumerate(HALVES if i < 3 else LAST)
    ]
    for m in range(HELD):
        if m % 2 == 0:
            loads[m // 2].wait()
        z_copies[m].start()
    loads[3].wait()

    @pl.when(core == 0)
    def _():
        for copy in z_copies[HELD:]:
            copy.start()

    load_a.wait()
    a_copy = remote(a_own, a_other, core_send, core_recv, device(half, z, y, x, 1 - core))
    a_copy.start()

    def prepare(source, which):
        def block_of(block, masked):
            at = block * BLK if masked else pl.multiple_of(block * BLK, BLK)
            for owner in range(4):
                lanes = pl.ds(at, EF - at if masked else BLK)
                if owner < 3:
                    part = source[pl.ds(owner * OWN, BLK), lanes]
                else:
                    part = pltpu.roll(source[pl.ds(ROWS - BLK, BLK), lanes], OWN, 0)
                if masked:
                    part = jnp.pad(part, ((0, 0), (0, KP - EF)))
                high, low = split(jnp.transpose(part))
                lanes = pl.ds(owner * WIDE + which * BLK, BLK)
                a_high[pl.ds(at, BLK), lanes] = high
                a_low[pl.ds(at, BLK), lanes] = low

        @pl.loop(0, KP // BLK - 1)
        def _(block):
            block_of(block, False)

        block_of(KP // BLK - 1, True)

    prepare(a_own, 0)
    for load in load_e:
        load.wait()
    denom_ref[...] = denominators(occ_ref[...].reshape(1, OCC), vir_ref[...].reshape(1, VIR), col, half, core * COLS + x * SLAB)
    a_copy.wait_recv()
    prepare(a_other, 1)

    def z_of(which):
        return 2 * half + lax.rem(core + which, 2)

    def multiply(source, kind, m, distance, first, tiles, direct=False):
        x_to = lax.rem(x + distance, 4)
        at = first * TILE
        if not isinstance(at, int):
            at = pl.multiple_of(at, TILE)
        cols = pl.ds(at, tiles * TILE)
        b = jnp.pad(source[x_to, cols, :], ((0, 0), (0, KP - EF)))
        b_high = b.astype(BF16).astype(F32)
        both = jnp.concatenate([b_high, b - b_high], axis=0).astype(BF16)
        for step in (2, 1, 3, 0):
            y_to = lax.rem(y + step, 4)
            lanes = pl.ds(pl.multiple_of(y_to * WIDE, WIDE), WIDE)
            upper = jnp.dot(both, a_high[:, lanes], preferred_element_type=F32)
            lower = jnp.dot(both, a_low[:, lanes], preferred_element_type=F32)
            n = tiles * TILE
            outgoing[kind, x_to, y_to, cols, :] = upper[:n] + (upper[n:] + (lower[:n] + lower[n:]))

            def send():
                remote(
                    outgoing.at[kind, x_to, y_to, cols], incoming.at[kind, plane, cols],
                    xy_send.at[m], xy_recv.at[m], device(half, z, y_to, x_to),
                ).start()

            if direct:
                for which in range(2):
                    remote(
                        outgoing.at[kind, x_to, y_to, cols, pl.ds(which * BLK, BLK)], direct_in.at[y * 4 + z],
                        direct_send, direct_recv, device(far, z_of(which), y_to, x),
                    ).start()
            elif step:
                send()
            elif isinstance(distance, int):
                incoming[kind, plane, cols, :] = outgoing[kind, x_to, y_to, cols, :]
            else:

                @pl.when(distance == 0)
                def _():
                    incoming[kind, plane, cols, :] = outgoing[kind, x_to, y_to, cols, :]

                @pl.when(distance != 0)
                def _():
                    send()

    def xy_all(kind, m, tiles, count):
        blocks = (kind, pl.ds(0, count), pl.ds(0, tiles * TILE))
        return remote(incoming.at[blocks], incoming.at[blocks], xy_send.at[m], xy_recv.at[m], device(far, z, y, x))

    def end_copy(kind, which, cols):
        z_to = z_of(which)
        half_to = far if kind else half
        return z_to, lambda: remote(
            reduced.at[kind, which, cols], landed.at[z, cols], end_send, end_recv, device(half_to, z_to, y, x)
        ).start()

    @pl.loop(0, 4)
    def _(i):
        multiply(b_own, 0, LOCAL + i, far_first(i), 0, 6)

    def finish_local():
        for i in range(4):
            xy_all(0, LOCAL + i, 6, 4 if i < 3 else 3).wait_recv()
        total = jnp.sum(incoming[0], axis=0)
        for which in range(2):
            reduced[0, which] = total[:, which * BLK : which * BLK + BLK]
        for which in range(2):
            z_to, send = end_copy(0, which, pl.ds(0, SLAB))

            @pl.when(z_to == z)
            def _():
                landed[z] = reduced[0, which]

            @pl.when(z_to != z)
            def _():
                send()

    @pl.loop(0, 7)
    def _(m):
        i = m // 2
        z_copy(m, far_first(i), 0, 3).wait_recv()
        @pl.when((core == 1) & (m == HELD - 1))
        def _():
            for copy in z_copies[HELD:]:
                copy.start()

        multiply(b_far, 1, m, far_first(i), 3 * lax.rem(m, 2), 3)

        @pl.when(m == 2)
        def _():
            finish_local()

    def slot(step):
        return lax.rem(x + step, 4) * 4

    for m in range(6):
        xy_all(1, m, 3, 4).wait_recv()
    total = jnp.sum(incoming[1, pl.ds(slot(1), 4)], axis=0)
    for step in (2, 3):
        total += jnp.sum(incoming[1, pl.ds(slot(step), 4)], axis=0)
    partial[...] = total

    def finish(j):
        first, tiles = LAST[j]
        cols = pl.ds(first * TILE, tiles * TILE)
        xy_all(1, 6 + j, tiles, 3).wait_recv()
        total = partial[cols, :] + jnp.sum(incoming[1, pl.ds(slot(0), 4), cols], axis=0)
        for which in range(2):
            lanes = slice(which * BLK, which * BLK + BLK)
            reduced[1, which, cols, :] = total[:, lanes]
            if j == 0:
                reduced[1, which, TAIL, :] = partial[TAIL, lanes]
        for which in range(2):
            end_copy(1, which, cols)[1]()
            if j == 0:
                end_copy(1, which, pl.ds(TAIL.start, SLAB - TAIL.start))[1]()

    for j in (1, 2):
        z_copies[6 + j].wait_recv()
        multiply(b_far, 1, 6 + j, 0, *LAST[j], direct=j == 2)
        if j == 1:
            finish(0)
    finish(1)

    def end_all(count):
        blocks = landed.at[pl.ds(0, count)]
        return remote(blocks, blocks, end_send, end_recv, device(far, z, y, x))

    def direct_all(count):
        blocks = direct_in.at[pl.ds(0, count)]
        return remote(blocks, blocks, direct_send, direct_recv, device(far, z, y, x))

    home = z // 2 == half

    @pl.when(home)
    def _():
        end_all(3).wait_recv()
        ladder_ref[...] = jnp.sum(landed[...], axis=0)

    @pl.when(jnp.logical_not(home))
    def _():
        end_all(4).wait_recv()
        ladder_ref[...] = jnp.sum(landed[...], axis=0)
        direct_all(16).wait_recv()
        ladder_ref[TAIL, :] += jnp.sum(direct_in[...], axis=0)

    a_copy.wait_send()
    for copy in z_copies:
        copy.wait_send()
    for m in range(PIECES - 1):
        xy_all(1, m, 3 if m < 6 else LAST[m - 6][1], 4 if m < 6 else 3).wait_send()
    direct_all(8).wait_send()
    for i in range(4):
        xy_all(0, LOCAL + i, 6, 4 if i < 3 else 3).wait_send()
    end_all(3).wait_send()

    @pl.when(jnp.logical_not(home))
    def _():
        end_all(1).wait_send()


def shards(amplitudes, integrals, occ_energy, vir_energy):
    block = jax.ShapeDtypeStruct((SLAB, BLK), F32)
    dma = pltpu.SemaphoreType.DMA
    vmem = pl.BlockSpec(memory_space=pltpu.VMEM)
    hbm = pl.BlockSpec(memory_space=pltpu.HBM)
    ladder, denominator = pl.pallas_call(
        kernel,
        out_shape=(block, block),
        in_specs=[hbm] * 4,
        out_specs=(vmem, vmem),
        scratch_shapes=[
            pltpu.VMEM((ROWS, EF), F32),
            pltpu.VMEM((ROWS, EF), F32),
            pltpu.VMEM((KP, 4 * WIDE), BF16),
            pltpu.VMEM((KP, 4 * WIDE), BF16),
            pltpu.VMEM((4, SLAB, EF), F32),
            pltpu.VMEM((4, SLAB, EF), F32),
            pltpu.VMEM((2, 4, 4, SLAB, WIDE), F32),
            pltpu.VMEM((2, 16, SLAB, WIDE), F32),
            pltpu.VMEM((SLAB, WIDE), F32),
            pltpu.VMEM((2, 2, SLAB, BLK), F32),
            pltpu.VMEM((4, SLAB, BLK), F32),
            pltpu.VMEM((16, TILE * LAST[2][1], BLK), F32),
            pltpu.VMEM((OCC,), F32),
            pltpu.VMEM((VIR,), F32),
            dma, dma((4,)), dma((2,)), dma, dma,
            dma((PIECES,)), dma((PIECES,)),
            dma((PIECES + 4,)), dma((PIECES + 4,)),
            dma, dma, dma, dma,
        ],
        compiler_params=pltpu.CompilerParams(collective_id=0, has_side_effects=True, vmem_limit_bytes=20 * 2**20),
    )(*[pltpu.with_memory_space_constraint(v, pltpu.HBM) for v in (amplitudes, integrals.T.reshape(4, SLAB, EF), occ_energy, vir_energy)])
    ladder = ladder[:, :OWN].T
    return ladder, ladder / denominator[:, :OWN].T


def solution(mesh):
    in_specs = (P("row", ("layer", "col")), P(("layer", "col"), "row"), P(), P())
    out_specs = (P("col", ("row", "layer")), P("col", ("row", "layer")))
    return jax.shard_map(shards, mesh=mesh, in_specs=in_specs, out_specs=out_specs, check_vma=False)
```
